32 devices in a mesh: dom: 32 (over z, y, x, core).
Axes of the slice: x: 2, y: 2, z: 4, core: 2. Of those that a mesh axis runs over, the one named last changes fastest.
Arguments:
- tracer: float32 [40, 32768], P(None, 'dom'), may hold values from -6 to 6
- bottom_levels: int32 [32768], P('dom'), may hold values from 1 to 40
- neighbours: int32 [6, 32768], P(None, 'dom'), may hold values from 0 to 2048, as said below
- edge_weight: float32 [6, 32768], P(None, 'dom'), may hold values from 0.05 to 0.5
- ssh: float32 [32768], P('dom'), may hold values from -6 to 6
- velocity: float32 [32768], P('dom'), may hold values from -3 to 3
- send_blocks: int32 [32, 4, 2], P('dom'), may hold values from -1 to 7
- thickness: float32 [40], replicated, may hold values from 0.5 to 4
- profile: float32 [40], replicated, may hold values from -4 to 4
Outputs:
- tracer_out: float32 [40, 32768], P(None, 'dom')
- ssh_out: float32 [32768], P('dom')
- velocity_out: float32 [32768], P('dom')
The draws below stay inside these ranges and needn't reach their ends.
Inputs may be any that keep to these rules, and one draw needn't show every extreme that they name: `neighbours`: entries 0 to 1023 are the partition's own cells, the next 1024 its received halo cells in the order of ext, and 2048 is land. `send_blocks`: -1 marks an empty slot; other entries are block numbers within the sending partition.
All inputs are finite; a program needn't handle non-finite values.
Results may differ from the reference program's by a relative error of at most 0.0003.
Values sent between devices are 32-bit elements; how exact they have to be, the bound alone decides.
No kernel may reach another device: no remote copies, remote signals or barrier semaphores. Data moves between devices by JAX's collectives and lax.ppermute only.
A program may use at most 64 MiB of HBM per device.

```python
import math
import jax
import jax.numpy as jnp

BLOCK = 128
BLK_DEV = 8
LEV = 40
SEND = 2
SUBSTEPS = 6
CELLS_DEV = 1024
HALO = 1024
TOTAL_CELLS = 32768
N_DOM = 32


def draw_neighbours(key, part):
    first_key, second_key, third_key = jax.random.split(jax.random.fold_in(key, 11), 3)
    shape = (6, TOTAL_CELLS)
    kinds = jax.random.randint(first_key, shape, 0, 20)
    position = jnp.arange(TOTAL_CELLS, dtype=jnp.int32)[None, :] % CELLS_DEV
    nearby = jnp.clip(position + jax.random.randint(second_key, shape, -256, 257), 0, CELLS_DEV - 1)
    remote = CELLS_DEV + jax.random.randint(third_key, shape, 0, HALO)
    landed = jnp.full(shape, CELLS_DEV + HALO, jnp.int32)
    return jnp.where(kinds == 0, landed, jnp.where(kinds <= 4, remote, nearby)).astype(jnp.int32)


def touch_ends(array, stream_key, smallest, largest):
    extent = array.shape
    index_at = [jax.random.randint(jax.random.fold_in(stream_key, axis), (), 0, extent[axis]) for axis in range(len(extent))]
    array = array.at[tuple(index_at)].set(smallest)
    longest = extent.index(max(extent))
    index_at[longest] = (index_at[longest] + 1) % extent[longest]
    return array.at[tuple(index_at)].set(largest)


def shard_levels(own_key, dims, cuts, smallest, largest):
    factor_of, own = 1.0, jax.random.fold_in(own_key, 6)
    for dim, shards_of in cuts:
        steps = jnp.exp(jax.random.uniform(jax.random.fold_in(own, dim), (shards_of,), jnp.float32, smallest / len(cuts), largest / len(cuts)))
        factor_of = factor_of * jnp.repeat(steps, dims[dim] // shards_of).reshape([-1 if axis == dim else 1 for axis in range(len(dims))])
    return factor_of


def gaussian(key, dims, deviation, limit, cuts=(), kind=jnp.bfloat16):
    drawn = deviation * jax.random.normal(key, dims, jnp.float32)
    if cuts:
        drawn = drawn * shard_levels(key, dims, cuts, -0.22, 0.18)
    return jnp.clip(drawn, -limit, limit).astype(kind)


def setup_inputs(seed: int = 0) -> dict:
    key_of = jax.random.split(jax.random.key(seed), 10)
    tracer = gaussian(key_of[0], (LEV, TOTAL_CELLS), 1.0, 6.0, ((1, 32),), jnp.float32)
    bottom_levels = touch_ends(jax.random.randint(key_of[1], (TOTAL_CELLS,), 1, LEV + 1), jax.random.fold_in(key_of[1], 1), 1, LEV).astype(jnp.int32)
    neighbours = draw_neighbours(jax.random.fold_in(key_of[9], 71), 0)
    edge_weight = jnp.clip(jnp.exp(math.log(0.5) - 2.3025851 * jax.random.uniform(key_of[3], (6, TOTAL_CELLS), jnp.float32) ** shard_levels(key_of[3], (6, TOTAL_CELLS), ((1, 32),), -0.2, 0.2)), 0.05, 0.5)
    ssh = gaussian(key_of[4], (TOTAL_CELLS,), 1.0, 6.0, ((0, 32),), jnp.float32)
    velocity = gaussian(key_of[5], (TOTAL_CELLS,), 0.5, 3.0, ((0, 32),), jnp.float32)
    send_blocks = touch_ends(jax.random.randint(key_of[6], (N_DOM, 4, SEND), -1, BLK_DEV), jax.random.fold_in(key_of[6], 1), -1, BLK_DEV - 1).astype(jnp.int32)
    thickness = jnp.clip(jnp.exp(jax.random.uniform(key_of[7], (LEV,), jnp.float32, math.log(0.5), math.log(4.0))), 0.5, 4.0)
    profile = gaussian(key_of[8], (LEV,), 1.0, 4.0, (), jnp.float32)
    return {"tracer": tracer, "bottom_levels": bottom_levels, "neighbours": neighbours, "edge_weight": edge_weight, "ssh": ssh, "velocity": velocity, "send_blocks": send_blocks, "thickness": thickness, "profile": profile}


OFFSETS = (1, -1, 2, -2)
horizontal_rate = 0.5
vertical_rate = 0.5
tracer_step = 0.2
barotropic_step = 0.5
friction = 0.05


def extend(field, send_blocks):
    cells = BLK_DEV * BLOCK
    leading = field.shape[:-1]
    blocks = field.reshape(leading + (N_DOM * BLK_DEV, BLOCK))
    owners = jnp.arange(N_DOM, dtype=jnp.int32)
    pieces = [field.reshape(leading + (N_DOM, cells))]
    for number in range(4):
        source = owners - OFFSETS[number]
        inside = (source >= 0) & (source < N_DOM)
        clipped = jnp.clip(source, 0, N_DOM - 1).astype(jnp.int32)
        chosen = send_blocks[clipped, number]
        living = (inside[:, None] & (chosen >= 0)).astype(field.dtype)
        global_index = (clipped[:, None] * BLK_DEV + jnp.maximum(chosen, 0)).astype(jnp.int32)
        taken = jnp.take(blocks, global_index.reshape(-1), axis=-2)
        taken = taken.reshape(leading + (N_DOM, SEND * BLOCK))
        pieces.append(taken * jnp.repeat(living, BLOCK, axis=1))
    pieces.append(jnp.zeros(leading + (N_DOM, BLOCK), field.dtype))
    return jnp.concatenate(pieces, axis=-1)


def reference(tracer, bottom_levels, neighbours, edge_weight, ssh, velocity, send_blocks, thickness, profile):
    cells = BLK_DEV * BLOCK
    levels_f = bottom_levels.astype(jnp.float32)
    ext_tracer = extend(tracer, send_blocks)
    ext_levels = extend(levels_f, send_blocks)
    own_tracer = tracer.reshape(LEV, N_DOM, cells)
    own_levels = levels_f.reshape(N_DOM, cells)
    level_index = jnp.arange(LEV).astype(jnp.float32)[:, None, None]
    active = (level_index < own_levels[None]).astype(jnp.float32)
    tables = neighbours.reshape(6, N_DOM, cells)
    weights = edge_weight.reshape(6, N_DOM, cells)
    horizontal = jnp.zeros_like(own_tracer)
    for column in range(6):
        index = tables[column]
        near_levels = jnp.take_along_axis(ext_levels, index, axis=-1)
        near_active = (level_index < near_levels[None]).astype(jnp.float32)
        wide_index = jnp.broadcast_to(index[None], (LEV, N_DOM, cells))
        near_tracer = jnp.take_along_axis(ext_tracer, wide_index, axis=-1)
        horizontal = horizontal + weights[column][None] * near_active * (near_tracer - own_tracer)
    horizontal = horizontal * active
    zero_level = jnp.zeros((1, N_DOM, cells), own_tracer.dtype)
    below = jnp.concatenate([active[1:] * (own_tracer[1:] - own_tracer[:-1]), zero_level], axis=0)
    above = jnp.concatenate([zero_level, active[:-1] * (own_tracer[:-1] - own_tracer[1:])], axis=0)
    vertical = active * (below + above)
    tendency = horizontal_rate * horizontal + vertical_rate * vertical
    layers = active * thickness[:, None, None]
    forcing = jnp.sum(layers * own_tracer, axis=0) / jnp.sum(layers, axis=0)
    height = ssh.reshape(N_DOM, cells)
    speed = velocity.reshape(N_DOM, cells)
    summed = jnp.zeros_like(speed)
    for counter in range(SUBSTEPS):
        extended = extend(height.reshape(-1), send_blocks)
        laplace = jnp.zeros_like(height)
        for column in range(6):
            near_height = jnp.take_along_axis(extended, tables[column], axis=-1)
            laplace = laplace + weights[column] * (near_height - height)
        speed = (1.0 - friction) * speed + barotropic_step * (laplace + forcing)
        height = height + barotropic_step * speed
        summed = summed + speed
    tracer_out = own_tracer + tracer_step * tendency + active * profile[:, None, None] * (summed / SUBSTEPS)[None]
    return tracer_out.reshape(LEV, N_DOM * cells), height.reshape(-1), speed.reshape(-1)
```

```python
import functools

import jax
import jax.numpy as jnp
from jax import lax
from jax.experimental import pallas as pl
from jax.experimental.pallas import tpu as pltpu
from jax.sharding import PartitionSpec as P

LANES = 128
SUBS = 8
SUBSTEPS = 6
OFFSETS = (1, -1, 2, -2)
horizontal_rate = 0.5
vertical_rate = 0.5
tracer_step = 0.2
barotropic_step = 0.5
friction = 0.05
ABSENT = 3e38
PRESENT = 1e38

SMEM = pl.BlockSpec(memory_space=pltpu.SMEM)
VMEM = pl.BlockSpec(memory_space=pltpu.VMEM)


def even_swap(count, by):
    return [(i, i ^ by) for i in range(count)]


def odd_swap(count, by):
    pairs = [(i, i + by) for i in range(by, count - by) if (i // by) % 2 == 1]
    pairs += [(b, a) for a, b in pairs]
    busy = {a for a, _ in pairs}
    rest = [i for i in range(count) if i not in busy]
    pairs += list(zip(rest[0::2], rest[1::2])) + list(zip(rest[1::2], rest[0::2]))
    return pairs


def exchange(payloads, count):
    ways = (even_swap(count, 1), odd_swap(count, 1), even_swap(count, 2), odd_swap(count, 2))
    return [lax.ppermute(value, "dom", way) for value, way in zip(payloads, ways)]


def column(scalars, tile):
    rows = lax.broadcasted_iota(jnp.int32, (SUBS, LANES), 0)
    value = jnp.zeros((SUBS, LANES), jnp.float32)
    for k in range(SUBS):
        value = jnp.where(rows == k, scalars[tile * SUBS + k], value)
    return value


def localize(index, place, count, cells, send):
    span = send * LANES
    result = index
    for g, offset in enumerate(OFFSETS):
        source = place - offset
        inside = jnp.logical_and(source >= 0, source < count)
        swapped = (place // abs(offset)) % 2 == 0
        step = jnp.where(swapped, span if g % 2 == 0 else -span, 0)
        low = cells + g * span
        mine = jnp.logical_and(index >= low, index < low + span)
        moved = jnp.where(inside, index + step, cells + 4 * span)
        result = jnp.where(mine, moved, result)
    return result


def chosen_slot(meta, way, slot, send):
    place = meta[0]
    offset = 1 if way < 2 else 2
    first = (place // offset) % 2 == 0
    base = 0 if way < 2 else 2
    near = meta[1 + (base + way % 2) * send + slot]
    far = meta[1 + (base + 1 - way % 2) * send + slot]
    return jnp.where(first, near, far)


def pick_rows(meta, field, outs, send, row=0):
    for way in range(4):
        for slot in range(send):
            block = chosen_slot(meta, way, slot, send)
            filled = (block >= 0).astype(jnp.float32)
            outs[way][row + slot : row + slot + 1, :] = (
                field[pl.ds(jnp.maximum(block, 0), 1), :] * filled
            )


def prepare(
    meta, thick, tracer, bottom, index, weight, ssh, forcing, index_out, weight_out, *outs,
    count, send,
):
    levels, cells = tracer.shape
    tiles = levels // SUBS
    blocks = cells // LANES
    rows = lax.broadcasted_iota(jnp.int32, (SUBS, LANES), 0)
    place = meta[0]
    thicks = [column(thick, k) for k in range(tiles)]
    for way in range(4):
        for slot in range(send):
            block = chosen_slot(meta, way, slot, send)
            safe = jnp.maximum(block, 0)
            depth = jnp.where(block >= 0, bottom[pl.ds(safe, 1), :], 0)
            at = pl.multiple_of(safe * LANES, LANES)
            for k in range(tiles):
                value = tracer[k * SUBS : (k + 1) * SUBS, pl.ds(at, LANES)]
                base = slot * levels + k * SUBS
                outs[way][base : base + SUBS, :] = jnp.where(rows + k * SUBS < depth, value, ABSENT)
    pick_rows(meta, ssh, outs, send, send * levels)
    for b in range(blocks):
        top = jnp.zeros((SUBS, LANES), jnp.float32)
        low = jnp.zeros((SUBS, LANES), jnp.float32)
        depth = bottom[b : b + 1, :]
        for k in range(tiles):
            layer = jnp.where(rows + k * SUBS < depth, thicks[k], 0.0)
            top = top + layer * tracer[k * SUBS : (k + 1) * SUBS, b * LANES : (b + 1) * LANES]
            low = low + layer
        forcing[b : b + 1, :] = jnp.sum(top, axis=0, keepdims=True) / jnp.sum(
            low, axis=0, keepdims=True
        )
    edges = index.shape[0]
    for b in range(blocks):
        for j in range(edges):
            row = index[j : j + 1, b * LANES : (b + 1) * LANES]
            index_out[j, b : b + 1, :] = row
            weight_out[j, b : b + 1, :] = weight[j : j + 1, b * LANES : (b + 1) * LANES]
    for j in range(edges):
        index_out[j] = localize(index_out[j], place, count, cells, send)


def advance(height, speed, total, forcing, index, weight, arrived, row, send):
    blocks = height.shape[0]
    own = height[...]
    laplace = jnp.zeros_like(own)
    for j in range(index.shape[0]):
        near = index[j]
        lane = jnp.bitwise_and(near, LANES - 1)
        block = jnp.right_shift(near, 7)
        got = jnp.zeros_like(own)
        for r in range(blocks + 4 * send):
            if r < blocks:
                source = height[r : r + 1, :]
            else:
                at = row + (r - blocks) % send
                source = arrived[(r - blocks) // send][at : at + 1, :]
            source = jnp.broadcast_to(source, own.shape)
            got = jnp.where(block == r, jnp.take_along_axis(source, lane, axis=1), got)
        laplace = laplace + weight[j] * (got - own)
    faster = (1.0 - friction) * speed[...] + barotropic_step * (laplace + forcing[...])
    return own + barotropic_step * faster, faster, total[...] + faster


def substep(
    meta, height, speed, total, forcing, index, weight, a, b, c, d, new_height, new_speed,
    new_total, *outs, row, send,
):
    new_height[...], new_speed[...], new_total[...] = advance(
        height, speed, total, forcing, index, weight, (a, b, c, d), row, send
    )
    pick_rows(meta, new_height, outs, send)


def last_substep(
    profile, height, speed, total, forcing, index, weight, a, b, c, d, bottom, base, new_height,
    new_speed, out, mean, *, row, send,
):
    new_height[...], new_speed[...], whole = advance(
        height, speed, total, forcing, index, weight, (a, b, c, d), row, send
    )
    mean[...] = whole / SUBSTEPS
    rows = lax.broadcasted_iota(jnp.int32, (SUBS, LANES), 0)
    for k in range(out.shape[0] // SUBS):
        shape = column(profile, k)
        for i in range(out.shape[1] // LANES):
            at = (slice(k * SUBS, (k + 1) * SUBS), slice(i * LANES, (i + 1) * LANES))
            added = jnp.where(rows + k * SUBS < bottom[i : i + 1, :], shape, 0.0)
            out[at] = base[at] + added * mean[i : i + 1, :]


def tracer_base(
    meta, tracer, bottom, index, weight, a, b, c, d, out, held, *, count, send
):
    levels, cells = tracer.shape
    tiles = levels // SUBS
    blocks = cells // LANES
    edges = index.shape[0]
    arrived = (a, b, c, d)
    rows = lax.broadcasted_iota(jnp.int32, (SUBS, LANES), 0)
    place = meta[0]
    for i in range(blocks):
        depth = bottom[i : i + 1, :]
        for k in range(tiles):
            at = (slice(k * SUBS, (k + 1) * SUBS), slice(i * LANES, (i + 1) * LANES))
            held[at] = jnp.where(rows + k * SUBS < depth, tracer[at], ABSENT)

    def cell_block(i, carry):
        at = pl.multiple_of(i * LANES, LANES)
        lanes = pl.ds(at, LANES)
        depth = bottom[pl.ds(i, 1), :]
        mine = [tracer[k * SUBS : (k + 1) * SUBS, lanes] for k in range(tiles)]
        flat = [jnp.zeros((SUBS, LANES), jnp.float32) for _ in range(tiles)]
        for j in range(edges):
            near = localize(index[j : j + 1, lanes], place, count, cells, send)
            near = jnp.broadcast_to(near, (SUBS, LANES))
            lane = jnp.bitwise_and(near, LANES - 1)
            block = jnp.right_shift(near, 7)
            factor = weight[j : j + 1, lanes]
            got = [jnp.full((SUBS, LANES), ABSENT, jnp.float32) for _ in range(tiles)]
            for r in range(blocks + 4 * send):
                here = block == r
                for k in range(tiles):
                    if r < blocks:
                        source = held[k * SUBS : (k + 1) * SUBS, r * LANES : (r + 1) * LANES]
                    else:
                        base = (r - blocks) % send * levels + k * SUBS
                        source = arrived[(r - blocks) // send][base : base + SUBS, :]
                    got[k] = jnp.where(here, jnp.take_along_axis(source, lane, axis=1), got[k])
            for k in range(tiles):
                flat[k] = flat[k] + factor * jnp.where(got[k] < PRESENT, got[k] - mine[k], 0.0)
        for k in range(tiles):
            first = rows + k * SUBS
            value = mine[k]
            up = pltpu.roll(value, SUBS - 1, 0)
            if k + 1 < tiles:
                up = jnp.where(rows == SUBS - 1, pltpu.roll(mine[k + 1], SUBS - 1, 0), up)
            down = pltpu.roll(value, 1, 0)
            if k > 0:
                down = jnp.where(rows == 0, pltpu.roll(mine[k - 1], 1, 0), down)
            below = jnp.where(first + 1 < jnp.minimum(depth, levels), up - value, 0.0)
            above = jnp.where(first > 0, down - value, 0.0)
            active = first < depth
            moved = horizontal_rate * flat[k] + vertical_rate * (below + above)
            out[k * SUBS : (k + 1) * SUBS, lanes] = value + tracer_step * jnp.where(
                active, moved, 0.0
            )
        return carry

    lax.fori_loop(0, blocks, cell_block, 0)


def shards(
    tracer, bottom_levels, neighbours, edge_weight, ssh, velocity, send_blocks, thickness, profile
):
    count = lax.axis_size("dom")
    levels, cells = tracer.shape
    send = send_blocks.shape[-1]
    edges = neighbours.shape[0]
    blocks = cells // LANES
    tile = (blocks, LANES)
    place = lax.axis_index("dom").astype(jnp.int32)
    meta = jnp.concatenate([place[None], send_blocks.reshape(-1)])
    bottom = bottom_levels.reshape(tile)
    height = ssh.reshape(tile)
    speed = velocity.reshape(tile)
    cell = jax.ShapeDtypeStruct(tile, jnp.float32)
    packed = send * levels + SUBS
    small = jax.ShapeDtypeStruct((send, LANES), jnp.float32)
    forcing, index, weight, *out = pl.pallas_call(
        functools.partial(prepare, count=count, send=send),
        out_shape=[
            cell,
            jax.ShapeDtypeStruct((edges,) + tile, jnp.int32),
            jax.ShapeDtypeStruct((edges,) + tile, jnp.float32),
        ]
        + [jax.ShapeDtypeStruct((packed, LANES), jnp.float32)] * 4,
        in_specs=[SMEM, SMEM] + [VMEM] * 5,
        cost_estimate=pl.CostEstimate(flops=4000000, bytes_accessed=600000, transcendentals=0),
        name="prepare",
    )(meta, thickness, tracer, bottom, neighbours, edge_weight, height)
    first = exchange(out, count)
    base = pl.pallas_call(
        functools.partial(tracer_base, count=count, send=send),
        out_shape=jax.ShapeDtypeStruct(tracer.shape, jnp.float32),
        in_specs=[SMEM] + [VMEM] * 8,
        scratch_shapes=[pltpu.VMEM(tracer.shape, jnp.float32)],
        cost_estimate=pl.CostEstimate(flops=20000000, bytes_accessed=800000, transcendentals=0),
        name="tracer_base",
    )(meta, tracer, bottom, neighbours, edge_weight, *first)
    total = jnp.zeros(tile, jnp.float32)
    arrived = first
    for number in range(SUBSTEPS - 1):
        row = send * levels if number == 0 else 0
        height, speed, total, *out = pl.pallas_call(
            functools.partial(substep, row=row, send=send),
            out_shape=[cell] * 3 + [small] * 4,
            in_specs=[SMEM] + [VMEM] * 10,
            cost_estimate=pl.CostEstimate(flops=500000, bytes_accessed=100000, transcendentals=0),
            name="substep",
        )(meta, height, speed, total, forcing, index, weight, *arrived)
        arrived = exchange(out, count)
    height, speed, result = pl.pallas_call(
        functools.partial(last_substep, row=0, send=send),
        out_shape=[cell, cell, jax.ShapeDtypeStruct(tracer.shape, jnp.float32)],
        in_specs=[SMEM] + [VMEM] * 12,
        scratch_shapes=[pltpu.VMEM(tile, jnp.float32)],
        cost_estimate=pl.CostEstimate(flops=1000000, bytes_accessed=500000, transcendentals=0),
        name="last_substep",
    )(profile, height, speed, total, forcing, index, weight, *arrived, bottom, base)
    return (result, height.reshape(-1), speed.reshape(-1))


def solution(mesh):
    placed = (
        P(None, "dom"),
        P("dom"),
        P(None, "dom"),
        P(None, "dom"),
        P("dom"),
        P("dom"),
        P("dom", None, None),
        P(),
        P(),
    )
    return jax.shard_map(
        shards,
        mesh=mesh,
        in_specs=placed,
        out_specs=(P(None, "dom"), P("dom"), P("dom")),
        check_vma=False,
    )
```

```python
import functools

import jax
import jax.numpy as jnp
from jax import lax
from jax.experimental import pallas as pl
from jax.experimental.pallas import tpu as pltpu
from jax.sharding import PartitionSpec as P

LANES = 128
SUBS = 8
SUBSTEPS = 6
OFFSETS = (1, -1, 2, -2)
horizontal_rate = 0.5
vertical_rate = 0.5
tracer_step = 0.2
barotropic_step = 0.5
friction = 0.05
ABSENT = 3e38
PRESENT = 1e38

SMEM = pl.BlockSpec(memory_space=pltpu.SMEM)
VMEM = pl.BlockSpec(memory_space=pltpu.VMEM)


def even_swap(count, by):
    return [(i, i ^ by) for i in range(count)]


def odd_swap(count, by):
    pairs = [(i, i + by) for i in range(by, count - by) if (i // by) % 2 == 1]
    pairs += [(b, a) for a, b in pairs]
    busy = {a for a, _ in pairs}
    rest = [i for i in range(count) if i not in busy]
    pairs += list(zip(rest[0::2], rest[1::2])) + list(zip(rest[1::2], rest[0::2]))
    return pairs


def exchange(payloads, count):
    ways = (even_swap(count, 1), odd_swap(count, 1), even_swap(count, 2), odd_swap(count, 2))
    return [lax.ppermute(value, "dom", way) for value, way in zip(payloads, ways)]


def column(scalars, tile):
    rows = lax.broadcasted_iota(jnp.int32, (SUBS, LANES), 0)
    value = jnp.zeros((SUBS, LANES), jnp.float32)
    for k in range(SUBS):
        value = jnp.where(rows == k, scalars[tile * SUBS + k], value)
    return value


def localize(index, place, count, cells, send):
    span = send * LANES
    result = index
    for g, offset in enumerate(OFFSETS):
        source = place - offset
        inside = jnp.logical_and(source >= 0, source < count)
        swapped = (place // abs(offset)) % 2 == 0
        step = jnp.where(swapped, span if g % 2 == 0 else -span, 0)
        low = cells + g * span
        mine = jnp.logical_and(index >= low, index < low + span)
        moved = jnp.where(inside, index + step, cells + 4 * span)
        result = jnp.where(mine, moved, result)
    return result


def chosen_slot(meta, way, slot, send):
    place = meta[0]
    offset = 1 if way < 2 else 2
    first = (place // offset) % 2 == 0
    base = 0 if way < 2 else 2
    near = meta[1 + (base + way % 2) * send + slot]
    far = meta[1 + (base + 1 - way % 2) * send + slot]
    return jnp.where(first, near, far)


def pick_rows(meta, field, outs, send, row=0):
    for way in range(4):
        for slot in range(send):
            block = chosen_slot(meta, way, slot, send)
            filled = (block >= 0).astype(jnp.float32)
            outs[way][row + slot : row + slot + 1, :] = (
                field[pl.ds(jnp.maximum(block, 0), 1), :] * filled
            )


def prepare(
    meta, thick, tracer, bottom, index, weight, ssh, forcing, index_out, weight_out, *outs,
    count, send,
):
    levels, cells = tracer.shape
    tiles = levels // SUBS
    blocks = cells // LANES
    rows = lax.broadcasted_iota(jnp.int32, (SUBS, LANES), 0)
    place = meta[0]
    thicks = [column(thick, k) for k in range(tiles)]
    for way in range(4):
        for slot in range(send):
            block = chosen_slot(meta, way, slot, send)
            safe = jnp.maximum(block, 0)
            depth = jnp.where(block >= 0, bottom[pl.ds(safe, 1), :], 0)
            at = pl.multiple_of(safe * LANES, LANES)
            for k in range(tiles):
                value = tracer[k * SUBS : (k + 1) * SUBS, pl.ds(at, LANES)]
                base = slot * levels + k * SUBS
                outs[way][base : base + SUBS, :] = jnp.where(rows + k * SUBS < depth, value, ABSENT)
    pick_rows(meta, ssh, outs, send, send * levels)
    for b in range(blocks):
        top = jnp.zeros((SUBS, LANES), jnp.float32)
        low = jnp.zeros((SUBS, LANES), jnp.float32)
        depth = bottom[b : b + 1, :]
        for k in range(tiles):
            layer = jnp.where(rows + k * SUBS < depth, thicks[k], 0.0)
            top = top + layer * tracer[k * SUBS : (k + 1) * SUBS, b * LANES : (b + 1) * LANES]
            low = low + layer
        forcing[b : b + 1, :] = jnp.sum(top, axis=0, keepdims=True) / jnp.sum(
            low, axis=0, keepdims=True
        )
    edges = index.shape[0]
    for b in range(blocks):
        for j in range(edges):
            row = index[j : j + 1, b * LANES : (b + 1) * LANES]
            index_out[j, b : b + 1, :] = row
            weight_out[j, b : b + 1, :] = weight[j : j + 1, b * LANES : (b + 1) * LANES]
    for j in range(edges):
        index_out[j] = localize(index_out[j], place, count, cells, send)


def advance(height, speed, total, forcing, index, weight, arrived, row, send):
    blocks = height.shape[0]
    own = height[...]
    laplace = jnp.zeros_like(own)
    for j in range(index.shape[0]):
        near = index[j]
        lane = jnp.bitwise_and(near, LANES - 1)
        block = jnp.right_shift(near, 7)
        got = jnp.zeros_like(own)
        for r in range(blocks + 4 * send):
            if r < blocks:
                source = height[r : r + 1, :]
            else:
                at = row + (r - blocks) % send
                source = arrived[(r - blocks) // send][at : at + 1, :]
            source = jnp.broadcast_to(source, own.shape)
            got = jnp.where(block == r, jnp.take_along_axis(source, lane, axis=1), got)
        laplace = laplace + weight[j] * (got - own)
    faster = (1.0 - friction) * speed[...] + barotropic_step * (laplace + forcing[...])
    return own + barotropic_step * faster, faster, total[...] + faster


def substep(
    meta, height, speed, total, forcing, index, weight, a, b, c, d, new_height, new_speed,
    new_total, *outs, row, send,
):
    new_height[...], new_speed[...], new_total[...] = advance(
        height, speed, total, forcing, index, weight, (a, b, c, d), row, send
    )
    pick_rows(meta, new_height, outs, send)


def last_substep(
    profile, height, speed, total, forcing, index, weight, a, b, c, d, bottom, base, new_height,
    new_speed, out, mean, *, row, send,
):
    new_height[...], new_speed[...], whole = advance(
        height, speed, total, forcing, index, weight, (a, b, c, d), row, send
    )
    mean[...] = whole / SUBSTEPS
    rows = lax.broadcasted_iota(jnp.int32, (SUBS, LANES), 0)
    for k in range(out.shape[0] // SUBS):
        shape = column(profile, k)
        for i in range(out.shape[1] // LANES):
            at = (slice(k * SUBS, (k + 1) * SUBS), slice(i * LANES, (i + 1) * LANES))
            added = jnp.where(rows + k * SUBS < bottom[i : i + 1, :], shape, 0.0)
            out[at] = base[at] + added * mean[i : i + 1, :]


def tracer_base(
    meta, tracer, bottom, index, weight, a, b, c, d, out, held, *, count, send
):
    levels, cells = tracer.shape
    tiles = levels // SUBS
    blocks = cells // LANES
    edges = index.shape[0]
    arrived = (a, b, c, d)
    rows = lax.broadcasted_iota(jnp.int32, (SUBS, LANES), 0)
    place = meta[0]
    for i in range(blocks):
        depth = bottom[i : i + 1, :]
        for k in range(tiles):
            at = (slice(k * SUBS, (k + 1) * SUBS), slice(i * LANES, (i + 1) * LANES))
            held[at] = jnp.where(rows + k * SUBS < depth, tracer[at], ABSENT)

    def cell_block(i, carry):
        at = pl.multiple_of(i * LANES, LANES)
        lanes = pl.ds(at, LANES)
        depth = bottom[pl.ds(i, 1), :]
        mine = [tracer[k * SUBS : (k + 1) * SUBS, lanes] for k in range(tiles)]
        flat = [jnp.zeros((SUBS, LANES), jnp.float32) for _ in range(tiles)]
        for j in range(edges):
            near = localize(index[j : j + 1, lanes], place, count, cells, send)
            near = jnp.broadcast_to(near, (SUBS, LANES))
            lane = jnp.bitwise_and(near, LANES - 1)
            block = jnp.right_shift(near, 7)
            factor = weight[j : j + 1, lanes]
            got = [jnp.full((SUBS, LANES), ABSENT, jnp.float32) for _ in range(tiles)]
            for r in range(blocks + 4 * send):
                here = block == r
                for k in range(tiles):
                    if r < blocks:
                        source = held[k * SUBS : (k + 1) * SUBS, r * LANES : (r + 1) * LANES]
                    else:
                        base = (r - blocks) % send * levels + k * SUBS
                        source = arrived[(r - blocks) // send][base : base + SUBS, :]
                    got[k] = jnp.where(here, jnp.take_along_axis(source, lane, axis=1), got[k])
            for k in range(tiles):
                flat[k] = flat[k] + factor * jnp.where(got[k] < PRESENT, got[k] - mine[k], 0.0)
        for k in range(tiles):
            first = rows + k * SUBS
            value = mine[k]
            up = pltpu.roll(value, SUBS - 1, 0)
            if k + 1 < tiles:
                up = jnp.where(rows == SUBS - 1, pltpu.roll(mine[k + 1], SUBS - 1, 0), up)
            down = pltpu.roll(value, 1, 0)
            if k > 0:
                down = jnp.where(rows == 0, pltpu.roll(mine[k - 1], 1, 0), down)
            below = jnp.where(first + 1 < jnp.minimum(depth, levels), up - value, 0.0)
            above = jnp.where(first > 0, down - value, 0.0)
            active = first < depth
            moved = horizontal_rate * flat[k] + vertical_rate * (below + above)
            out[k * SUBS : (k + 1) * SUBS, lanes] = value + tracer_step * jnp.where(
                active, moved, 0.0
            )
        return carry

    lax.fori_loop(0, blocks, cell_block, 0)


def shards(
    tracer, bottom_levels, neighbours, edge_weight, ssh, velocity, send_blocks, thickness, profile
):
    count = lax.axis_size("dom")
    levels, cells = tracer.shape
    send = send_blocks.shape[-1]
    edges = neighbours.shape[0]
    blocks = cells // LANES
    tile = (blocks, LANES)
    place = lax.axis_index("dom").astype(jnp.int32)
    meta = jnp.concatenate([place[None], send_blocks.reshape(-1)])
    bottom = bottom_levels.reshape(tile)
    height = ssh.reshape(tile)
    speed = velocity.reshape(tile)
    cell = jax.ShapeDtypeStruct(tile, jnp.float32)
    packed = send * levels + SUBS
    small = jax.ShapeDtypeStruct((send, LANES), jnp.float32)
    forcing, index, weight, *out = pl.pallas_call(
        functools.partial(prepare, count=count, send=send),
        out_shape=[
            cell,
            jax.ShapeDtypeStruct((edges,) + tile, jnp.int32),
            jax.ShapeDtypeStruct((edges,) + tile, jnp.float32),
        ]
        + [jax.ShapeDtypeStruct((packed, LANES), jnp.float32)] * 4,
        in_specs=[SMEM, SMEM] + [VMEM] * 5,
        cost_estimate=pl.CostEstimate(flops=4000000, bytes_accessed=600000, transcendentals=0),
        name="prepare",
        compiler_params=pltpu.CompilerParams(vmem_limit_bytes=4 << 20),
    )(meta, thickness, tracer, bottom, neighbours, edge_weight, height)
    first = exchange(out, count)
    base = pl.pallas_call(
        functools.partial(tracer_base, count=count, send=send),
        out_shape=jax.ShapeDtypeStruct(tracer.shape, jnp.float32),
        in_specs=[SMEM] + [VMEM] * 8,
        scratch_shapes=[pltpu.VMEM(tracer.shape, jnp.float32)],
        cost_estimate=pl.CostEstimate(flops=20000000, bytes_accessed=800000, transcendentals=0),
        name="tracer_base",
        compiler_params=pltpu.CompilerParams(vmem_limit_bytes=4 << 20),
    )(meta, tracer, bottom, neighbours, edge_weight, *first)
    total = jnp.zeros(tile, jnp.float32)
    arrived = first
    for number in range(SUBSTEPS - 1):
        row = send * levels if number == 0 else 0
        height, speed, total, *out = pl.pallas_call(
            functools.partial(substep, row=row, send=send),
            out_shape=[cell] * 3 + [small] * 4,
            in_specs=[SMEM] + [VMEM] * 10,
            cost_estimate=pl.CostEstimate(flops=500000, bytes_accessed=100000, transcendentals=0),
            name="substep",
            compiler_params=pltpu.CompilerParams(vmem_limit_bytes=2 << 20),
        )(meta, height, speed, total, forcing, index, weight, *arrived)
        arrived = exchange(out, count)
    height, speed, result = pl.pallas_call(
        functools.partial(last_substep, row=0, send=send),
        out_shape=[cell, cell, jax.ShapeDtypeStruct(tracer.shape, jnp.float32)],
        in_specs=[SMEM] + [VMEM] * 12,
        scratch_shapes=[pltpu.VMEM(tile, jnp.float32)],
        cost_estimate=pl.CostEstimate(flops=1000000, bytes_accessed=500000, transcendentals=0),
        name="last_substep",
        compiler_params=pltpu.CompilerParams(vmem_limit_bytes=4 << 20),
    )(profile, height, speed, total, forcing, index, weight, *arrived, bottom, base)
    return (result, height.reshape(-1), speed.reshape(-1))


def solution(mesh):
    placed = (
        P(None, "dom"),
        P("dom"),
        P(None, "dom"),
        P(None, "dom"),
        P("dom"),
        P("dom"),
        P("dom", None, None),
        P(),
        P(),
    )
    return jax.shard_map(
        shards,
        mesh=mesh,
        in_specs=placed,
        out_specs=(P(None, "dom"), P("dom"), P("dom")),
        check_vma=False,
    )
```

```python
import functools

import jax
import jax.numpy as jnp
from jax import lax
from jax.experimental import pallas as pl
from jax.experimental.pallas import tpu as pltpu
from jax.sharding import PartitionSpec as P

LANES = 128
SUBS = 8
SUBSTEPS = 6
TEAM = 4
OFFSETS = (1, -1, 2, -2)
horizontal_rate = 0.5
vertical_rate = 0.5
tracer_step = 0.2
barotropic_step = 0.5
friction = 0.05
ABSENT = 3e38
PRESENT = 1e38

SMEM = pl.BlockSpec(memory_space=pltpu.SMEM)
VMEM = pl.BlockSpec(memory_space=pltpu.VMEM)
HBM = pl.BlockSpec(memory_space=pltpu.HBM)


def even_swap(count, by):
    return [(i, i ^ by) for i in range(count)]


def odd_swap(count, by):
    pairs = [(i, i + by) for i in range(by, count - by) if (i // by) % 2 == 1]
    pairs += [(b, a) for a, b in pairs]
    busy = {a for a, _ in pairs}
    rest = [i for i in range(count) if i not in busy]
    pairs += list(zip(rest[0::2], rest[1::2])) + list(zip(rest[1::2], rest[0::2]))
    return pairs


def column(scalars, tile):
    rows = lax.broadcasted_iota(jnp.int32, (SUBS, LANES), 0)
    value = jnp.zeros((SUBS, LANES), jnp.float32)
    for k in range(SUBS):
        value = jnp.where(rows == k, scalars[tile * SUBS + k], value)
    return value


def localize(index, place, count, cells, send):
    span = send * LANES
    result = index
    for g, offset in enumerate(OFFSETS):
        source = place - offset
        inside = jnp.logical_and(source >= 0, source < count)
        swapped = (place // abs(offset)) % 2 == 0
        step = jnp.where(swapped, span if g % 2 == 0 else -span, 0)
        low = cells + g * span
        mine = jnp.logical_and(index >= low, index < low + span)
        moved = jnp.where(inside, index + step, cells + 4 * span)
        result = jnp.where(mine, moved, result)
    return result


def group_of(rows, send):
    return rows // send


def blend(rows, send, parts):
    value = jnp.zeros((SUBS, LANES), jnp.float32)
    for g, part in parts.items():
        value = jnp.where(group_of(rows, send) == g, part, value)
    return value


def outgoing(field, slots):
    taken = jnp.take_along_axis(field, jnp.maximum(slots, 0), axis=0)
    return jnp.where(slots >= 0, taken, 0.0)


def prepare(
    place_ref, slots, thick, tracer_hbm, bottom_hbm, index_hbm, weight_hbm, ssh_hbm, velocity_hbm,
    near, side, far, odd, odd_side, mine, tracer, bottom, index, weight, ssh, velocity, sems,
    *, count, send,
):
    sources = (bottom_hbm, tracer_hbm, index_hbm, weight_hbm, ssh_hbm, velocity_hbm)
    targets = (bottom, tracer, index, weight, ssh, velocity)
    copies = [
        pltpu.make_async_copy(source, target, sems.at[n])
        for n, (source, target) in enumerate(zip(sources, targets))
    ]
    for copy in copies:
        copy.start()
    levels, cells = tracer.shape
    tiles = levels // SUBS
    blocks = cells // LANES
    edges = index.shape[0]
    rows = lax.broadcasted_iota(jnp.int32, (SUBS, LANES), 0)
    place = place_ref[0]
    thicks = [column(thick, k) for k in range(tiles)]
    sent = jnp.zeros((SUBS, LANES), jnp.float32)
    for g in range(4):
        for slot in range(send):
            sent = jnp.where(rows == g * send + slot, slots[0, slot, g].astype(jnp.float32), sent)
    team = (2 * edges + 3) * SUBS
    mine[team : team + SUBS, :] = sent
    copies[0].wait()
    copies[1].wait()
    for way, out in enumerate((near, odd, side, odd_side)):
        offset = 1 if way < 2 else 2
        first = (place // offset) % 2 == 0
        base = 0 if way < 2 else 2
        start = out.shape[0] - send * levels
        for slot in range(send):
            block = jnp.where(
                first, slots[0, slot, base + way % 2], slots[0, slot, base + 1 - way % 2]
            )
            safe = jnp.maximum(block, 0)
            depth = jnp.where(block >= 0, bottom[pl.ds(safe, 1), :], 0)
            at = pl.multiple_of(safe * LANES, LANES)
            for k in range(tiles):
                value = tracer[k * SUBS : (k + 1) * SUBS, pl.ds(at, LANES)]
                row = start + slot * levels + k * SUBS
                out[row : row + SUBS, :] = jnp.where(rows + k * SUBS < depth, value, ABSENT)
    for b in range(blocks):
        top = jnp.zeros((SUBS, LANES), jnp.float32)
        low = jnp.zeros((SUBS, LANES), jnp.float32)
        depth = bottom[b : b + 1, :]
        for k in range(tiles):
            layer = jnp.where(rows + k * SUBS < depth, thicks[k], 0.0)
            top = top + layer * tracer[k * SUBS : (k + 1) * SUBS, b * LANES : (b + 1) * LANES]
            low = low + layer
        row = 2 * edges * SUBS + b
        mine[row : row + 1, :] = jnp.sum(top, axis=0, keepdims=True) / jnp.sum(
            low, axis=0, keepdims=True
        )
    for copy in copies[2:]:
        copy.wait()
    for b in range(blocks):
        lanes = slice(b * LANES, (b + 1) * LANES)
        for j in range(edges):
            row = j * SUBS + b
            found = index[j : j + 1, lanes]
            mine[row : row + 1, :] = bounded(found, place, count, cells, send).astype(jnp.float32)
            row = (edges + j) * SUBS + b
            mine[row : row + 1, :] = weight[j : j + 1, lanes]
    row = (2 * edges + 1) * SUBS
    mine[row : row + SUBS, :] = velocity[...]
    mine[row + SUBS : row + 2 * SUBS, :] = ssh[...]
    for k in range(mine.shape[0] // SUBS):
        at = slice(k * SUBS, (k + 1) * SUBS)
        value = mine[at, :]
        near[at, :] = value
        side[at, :] = value
        far[at, :] = value


def bounded(index, place, count, cells, send):
    span = send * LANES
    result = index
    for g, offset in enumerate(OFFSETS):
        source = place - offset
        inside = jnp.logical_and(source >= 0, source < count)
        low = jnp.where(inside, cells + 4 * span, cells + g * span)
        mine = jnp.logical_and(index >= low, index < cells + (g + 1) * span)
        result = jnp.where(mine, cells + 4 * span, result)
    return result


def gathered(rows_of, index, weight, own, pairs):
    laplace = jnp.zeros_like(own)
    for j in range(len(index)):
        lane = jnp.bitwise_and(index[j], LANES - 1)
        block = jnp.right_shift(index[j], 7)
        got = jnp.zeros_like(own)
        for r in range(pairs):
            got = jnp.where(block == r, jnp.take_along_axis(rows_of(r), lane, axis=1), got)
        laplace = laplace + weight[j] * (got - own)
    return laplace


def stepped(laplace, forcing, own, speed):
    faster = (1.0 - friction) * speed + barotropic_step * (laplace + forcing)
    return own + barotropic_step * faster, faster


def pack_edges(heights, speeds, slots, rows, send, even, way_even, way_odd):
    out = [outgoing(h, s) for h, s in zip(heights, slots)]
    fast = [outgoing(v, slots[q]) for q, v in enumerate(speeds)]
    right = [
        heights[3],
        heights[2],
        blend(rows, send, {0: out[2], 2: out[1]}),
        blend(rows, send, {0: out[1], 1: out[3], 2: out[0]}),
        edge_rows(out[3], out[2], rows, send, True),
        edge_rows(fast[3], fast[2], rows, send, True),
    ]
    left = [
        heights[0],
        heights[1],
        blend(rows, send, {1: out[1], 3: out[2]}),
        blend(rows, send, {0: out[0], 1: out[2], 3: out[3]}),
        edge_rows(out[0], out[1], rows, send, False),
        edge_rows(fast[0], fast[1], rows, send, False),
    ]
    for k in range(len(right)):
        at = slice(k * SUBS, (k + 1) * SUBS)
        way_even[at, :] = jnp.where(even, right[k], left[k])
        way_odd[at, :] = jnp.where(even, left[k], right[k])


def edge_rows(inner, outer, rows, send, rightward):
    if rightward:
        return jnp.where(group_of(rows, send) == 3, pltpu.roll(outer, send, 0), inner)
    return jnp.where(group_of(rows, send) == 2, pltpu.roll(outer, SUBS - send, 0), inner)


def gather_team(
    place_ref, mine, near, side, far, index, weight, force, slots, height, speed, way_even, way_odd,
    *, send,
):
    edges = index.shape[1]
    place = place_ref[0]
    position = place % TEAM
    even = (place // TEAM) % 2 == 0
    rows = lax.broadcasted_iota(jnp.int32, (SUBS, LANES), 0)
    for flip, ref in enumerate((mine, near, side, far)):
        q = jnp.bitwise_xor(position, flip)
        for j in range(edges):
            index[q, j] = ref[j * SUBS : (j + 1) * SUBS, :].astype(jnp.int32)
            weight[q, j] = ref[(edges + j) * SUBS : (edges + j + 1) * SUBS, :]
        row = 2 * edges * SUBS
        force[q] = ref[row : row + SUBS, :]
        speed[q] = ref[row + SUBS : row + 2 * SUBS, :]
        height[q] = ref[row + 2 * SUBS : row + 3 * SUBS, :]
        slots[q] = ref[row + 3 * SUBS : row + 4 * SUBS, :].astype(jnp.int32)
    held = [slots[q] for q in range(TEAM)]
    pack_edges(
        [height[q] for q in range(TEAM)], [speed[q] for q in range(TEAM)], held, rows, send, even,
        way_even, way_odd,
    )

    def both(k, field):
        at = slice((6 + k) * SUBS, (7 + k) * SUBS)
        picked = [outgoing(field(q), held[q]) for q in range(TEAM)]
        right = edge_rows(picked[3], picked[2], rows, send, True)
        left = edge_rows(picked[0], picked[1], rows, send, False)
        way_even[at, :] = jnp.where(even, right, left)
        way_odd[at, :] = jnp.where(even, left, right)

    for j in range(edges):
        both(j, lambda q: index[q, j].astype(jnp.float32))
        both(edges + j, lambda q: weight[q, j])
    both(2 * edges, lambda q: force[q])


def double_step(
    place, index, weight, force, slots, height_in, speed_in, total_in, even_in, odd_in, first_even,
    first_odd, height, speed, total, ext, virtual, outer, *, send,
):
    edges = index.shape[1]
    even = (place // TEAM) % 2 == 0
    rows = lax.broadcasted_iota(jnp.int32, (SUBS, LANES), 0)
    held = [slots[q] for q in range(TEAM)]

    def side_of(k, constant, right):
        ref_even, ref_odd = (first_even, first_odd) if constant else (even_in, odd_in)
        at = slice(k * SUBS, (k + 1) * SUBS)
        a, b = ref_even[at, :], ref_odd[at, :]
        return jnp.where(even, a, b) if right else jnp.where(even, b, a)

    def fill(heights, left, right):
        out = [outgoing(h, s) for h, s in zip(heights, held)]
        halos = (
            {0: left, 1: out[1], 2: pltpu.roll(left, SUBS - send, 0), 3: out[2]},
            {0: out[0], 1: out[2], 2: left, 3: out[3]},
            {0: out[1], 1: out[3], 2: out[0], 3: right},
            {0: out[2], 1: right, 2: out[1], 3: pltpu.roll(right, send, 0)},
        )
        for q in range(TEAM):
            ext[q, 0:SUBS, :] = heights[q]
            ext[q, SUBS : 2 * SUBS, :] = blend(rows, send, halos[q])
        return out

    def advance_team(heights, speeds):
        moved = []
        for q in range(TEAM):
            laplace = gathered(
                lambda r: jnp.broadcast_to(ext[q, r : r + 1, :], (SUBS, LANES)),
                [index[q, j] for j in range(edges)],
                [weight[q, j] for j in range(edges)],
                heights[q],
                2 * SUBS,
            )
            moved.append(stepped(laplace, force[q], heights[q], speeds[q]))
        return [m[0] for m in moved], [m[1] for m in moved]

    heights = [height_in[q] for q in range(TEAM)]
    speeds = [speed_in[q] for q in range(TEAM)]
    edge = [side_of(4, False, right) for right in (False, True)]
    out = fill(heights, edge[0], edge[1])
    virtual[0, 0:SUBS, :] = side_of(0, False, False)
    virtual[0, SUBS : 2 * SUBS, :] = side_of(2, False, False) + blend(
        rows, send, {1: out[0], 3: out[1]}
    )
    virtual[1, 0:SUBS, :] = side_of(1, False, False)
    virtual[1, SUBS : 2 * SUBS, :] = side_of(3, False, False) + blend(rows, send, {3: out[0]})
    virtual[2, 0:SUBS, :] = side_of(0, False, True)
    virtual[2, SUBS : 2 * SUBS, :] = side_of(2, False, True) + blend(
        rows, send, {0: out[3], 2: out[2]}
    )
    virtual[3, 0:SUBS, :] = side_of(1, False, True)
    virtual[3, SUBS : 2 * SUBS, :] = side_of(3, False, True) + blend(rows, send, {2: out[3]})
    later, faster = advance_team(heights, speeds)
    for number, right in enumerate((False, True)):
        moved_group = 2 if right else 3
        laplace = gathered(
            lambda r: jnp.where(
                group_of(rows, send) == moved_group,
                virtual[2 * number + 1, r : r + 1, :],
                virtual[2 * number, r : r + 1, :],
            ),
            [side_of(6 + j, True, right).astype(jnp.int32) for j in range(edges)],
            [side_of(6 + edges + j, True, right) for j in range(edges)],
            edge[number],
            2 * SUBS,
        )
        edge[number] = stepped(
            laplace, side_of(6 + 2 * edges, True, right), edge[number], side_of(5, False, right)
        )[0]
    fill(later, edge[0], edge[1])
    last, fastest = advance_team(later, faster)
    for q in range(TEAM):
        height[q] = last[q]
        speed[q] = fastest[q]
        before = 0.0 if total_in is None else total_in[q]
        total[q] = before + faster[q] + fastest[q]
    return last, fastest, held, rows, even


def first_pair(
    place, index, weight, force, slots, height_in, speed_in, even_in, odd_in, height, speed, total,
    way_even, way_odd, ext, virtual, *, send,
):
    last, fastest, held, rows, even = double_step(
        place[0], index, weight, force, slots, height_in, speed_in, None, even_in, odd_in, even_in,
        odd_in, height, speed, total, ext, virtual, None, send=send,
    )
    pack_edges(last, fastest, held, rows, send, even, way_even, way_odd)


def middle_pair(
    place, index, weight, force, slots, height_in, speed_in, total_in, even_in, odd_in, first_even,
    first_odd, height, speed, total, way_even, way_odd, ext, virtual, *, send,
):
    last, fastest, held, rows, even = double_step(
        place[0], index, weight, force, slots, height_in, speed_in, total_in, even_in, odd_in,
        first_even, first_odd, height, speed, total, ext, virtual, None, send=send,
    )
    pack_edges(last, fastest, held, rows, send, even, way_even, way_odd)


def last_pair(
    place, profile, index, weight, force, slots, height_in, speed_in, total_in, even_in, odd_in,
    first_even, first_odd, bottom, base, new_height, new_speed, out, height, speed, total, ext,
    virtual, *, send,
):
    double_step(
        place[0], index, weight, force, slots, height_in, speed_in, total_in, even_in, odd_in,
        first_even, first_odd, height, speed, total, ext, virtual, None, send=send,
    )
    position = place[0] % TEAM
    new_height[...] = height[position]
    new_speed[...] = speed[position]
    ext[0, 0:SUBS, :] = total[position] / SUBSTEPS
    rows = lax.broadcasted_iota(jnp.int32, (SUBS, LANES), 0)
    for k in range(out.shape[0] // SUBS):
        shape = column(profile, k)
        for i in range(out.shape[1] // LANES):
            at = (slice(k * SUBS, (k + 1) * SUBS), slice(i * LANES, (i + 1) * LANES))
            added = jnp.where(rows + k * SUBS < bottom[i : i + 1, :], shape, 0.0)
            out[at] = base[at] + added * ext[0, i : i + 1, :]


def tracer_base(meta, tracer, bottom, index, weight, a, b, c, d, out, held, *, count, send):
    levels, cells = tracer.shape
    tiles = levels // SUBS
    blocks = cells // LANES
    edges = index.shape[0]
    arrived = (a, b, c, d)
    rows = lax.broadcasted_iota(jnp.int32, (SUBS, LANES), 0)
    place = meta[0]
    for i in range(blocks):
        depth = bottom[i : i + 1, :]
        for k in range(tiles):
            at = (slice(k * SUBS, (k + 1) * SUBS), slice(i * LANES, (i + 1) * LANES))
            held[at] = jnp.where(rows + k * SUBS < depth, tracer[at], ABSENT)

    def cell_block(i, carry):
        at = pl.multiple_of(i * LANES, LANES)
        lanes = pl.ds(at, LANES)
        depth = bottom[pl.ds(i, 1), :]
        mine = [tracer[k * SUBS : (k + 1) * SUBS, lanes] for k in range(tiles)]
        flat = [jnp.zeros((SUBS, LANES), jnp.float32) for _ in range(tiles)]
        for j in range(edges):
            near = localize(index[j : j + 1, lanes], place, count, cells, send)
            near = jnp.broadcast_to(near, (SUBS, LANES))
            lane = jnp.bitwise_and(near, LANES - 1)
            block = jnp.right_shift(near, 7)
            factor = weight[j : j + 1, lanes]
            got = [jnp.full((SUBS, LANES), ABSENT, jnp.float32) for _ in range(tiles)]
            for r in range(blocks + 4 * send):
                here = block == r
                for k in range(tiles):
                    if r < blocks:
                        source = held[k * SUBS : (k + 1) * SUBS, r * LANES : (r + 1) * LANES]
                    else:
                        ref = arrived[(r - blocks) // send]
                        start = ref.shape[0] - send * levels
                        row = start + (r - blocks) % send * levels + k * SUBS
                        source = ref[row : row + SUBS, :]
                    got[k] = jnp.where(here, jnp.take_along_axis(source, lane, axis=1), got[k])
            for k in range(tiles):
                flat[k] = flat[k] + factor * jnp.where(got[k] < PRESENT, got[k] - mine[k], 0.0)
        for k in range(tiles):
            first = rows + k * SUBS
            value = mine[k]
            up = pltpu.roll(value, SUBS - 1, 0)
            if k + 1 < tiles:
                up = jnp.where(rows == SUBS - 1, pltpu.roll(mine[k + 1], SUBS - 1, 0), up)
            down = pltpu.roll(value, 1, 0)
            if k > 0:
                down = jnp.where(rows == 0, pltpu.roll(mine[k - 1], 1, 0), down)
            below = jnp.where(first + 1 < jnp.minimum(depth, levels), up - value, 0.0)
            above = jnp.where(first > 0, down - value, 0.0)
            moved = horizontal_rate * flat[k] + vertical_rate * (below + above)
            out[k * SUBS : (k + 1) * SUBS, lanes] = value + tracer_step * jnp.where(
                first < depth, moved, 0.0
            )
        return carry

    lax.fori_loop(0, blocks, cell_block, 0)


def shards(
    tracer, bottom_levels, neighbours, edge_weight, ssh, velocity, send_blocks, thickness, profile
):
    count = lax.axis_size("dom")
    levels, cells = tracer.shape
    send = send_blocks.shape[-1]
    edges = neighbours.shape[0]
    blocks = cells // LANES
    assert blocks == SUBS and 4 * send == SUBS and levels % SUBS == 0 and count % (2 * TEAM) == 0
    assert SUBSTEPS == 6
    tile = (blocks, LANES)
    place = lax.axis_index("dom").astype(jnp.int32)[None]
    slots = jnp.swapaxes(send_blocks, 1, 2)
    bottom = bottom_levels.reshape(tile)

    def shape(rows, kind=jnp.float32):
        return jax.ShapeDtypeStruct(rows, kind)

    def call(body, name, outs, ins, scratch, flops, limit=4):
        return pl.pallas_call(
            functools.partial(body, send=send),
            out_shape=outs,
            in_specs=ins,
            scratch_shapes=scratch,
            compiler_params=pltpu.CompilerParams(vmem_limit_bytes=limit << 20),
            cost_estimate=pl.CostEstimate(flops=flops, bytes_accessed=1000, transcendentals=0),
            name=name,
        )

    own = (2 * edges + 4) * SUBS
    halo = send * levels
    near, side, far, odd, odd_side, mine = call(
        functools.partial(prepare, count=count),
        "prepare",
        [
            shape((own + halo, LANES)),
            shape((own + halo, LANES)),
            shape((own, LANES)),
            shape((halo, LANES)),
            shape((halo, LANES)),
            shape((own, LANES)),
        ],
        [SMEM, SMEM, SMEM] + [HBM] * 6,
        [
            pltpu.VMEM(tracer.shape, jnp.float32),
            pltpu.VMEM(tile, jnp.int32),
            pltpu.VMEM(neighbours.shape, jnp.int32),
            pltpu.VMEM(edge_weight.shape, jnp.float32),
            pltpu.VMEM(tile, jnp.float32),
            pltpu.VMEM(tile, jnp.float32),
            pltpu.SemaphoreType.DMA((6,)),
        ],
        4000000,
    )(
        place, slots, thickness, tracer, bottom, neighbours, edge_weight, ssh.reshape(tile),
        velocity.reshape(tile),
    )
    side = lax.ppermute(side, "dom", even_swap(count, 2))
    far = lax.ppermute(far, "dom", even_swap(count, 3))
    near = lax.ppermute(near, "dom", even_swap(count, 1))
    odd = lax.ppermute(odd, "dom", odd_swap(count, 1))
    odd_side = lax.ppermute(odd_side, "dom", odd_swap(count, 2))

    def swap(pair):
        return (
            lax.ppermute(pair[0], "dom", even_swap(count, TEAM)),
            lax.ppermute(pair[1], "dom", odd_swap(count, TEAM)),
        )

    state = [shape((TEAM,) + tile)] * 2
    entire = (6 + 2 * edges + 1) * SUBS
    *tables, height, speed, way_even, way_odd = call(
        gather_team,
        "gather_team",
        [
            shape((TEAM, edges) + tile, jnp.int32),
            shape((TEAM, edges) + tile),
            shape((TEAM,) + tile),
            shape((TEAM,) + tile, jnp.int32),
        ]
        + state
        + [shape((entire, LANES))] * 2,
        [SMEM] + [VMEM] * 4,
        [],
        500000,
    )(place, mine, near, side, far)
    constant = swap((way_even, way_odd))
    base = call(
        functools.partial(tracer_base, count=count),
        "tracer_base",
        shape(tracer.shape),
        [SMEM] + [VMEM] * 8,
        [pltpu.VMEM(tracer.shape, jnp.float32)],
        20000000,
    )(place, tracer, bottom, neighbours, edge_weight, near, odd, side, odd_side)
    scratch = [pltpu.VMEM((TEAM, 2 * SUBS, LANES), jnp.float32)] * 2
    light = [shape((6 * SUBS, LANES))] * 2
    height, speed, total, *ways = call(
        first_pair, "first_pair", state + state[:1] + light, [SMEM] + [VMEM] * 8, scratch, 2000000
    )(place, *tables, height, speed, *constant)
    arrived = swap(ways)
    height, speed, total, *ways = call(
        middle_pair, "middle_pair", state + state[:1] + light, [SMEM] + [VMEM] * 11, scratch, 2000000
    )(place, *tables, height, speed, total, *arrived, *constant)
    arrived = swap(ways)
    team_scratch = [pltpu.VMEM((TEAM,) + tile, jnp.float32)] * 3
    height, speed, result = call(
        last_pair,
        "last_pair",
        [shape(tile), shape(tile), shape(tracer.shape)],
        [SMEM, SMEM] + [VMEM] * 13,
        team_scratch + scratch,
        2500000,
    )(place, profile, *tables, height, speed, total, *arrived, *constant, bottom, base)
    return (result, height.reshape(-1), speed.reshape(-1))


def solution(mesh):
    placed = (
        P(None, "dom"),
        P("dom"),
        P(None, "dom"),
        P(None, "dom"),
        P("dom"),
        P("dom"),
        P("dom", None, None),
        P(),
        P(),
    )
    return jax.shard_map(
        shards,
        mesh=mesh,
        in_specs=placed,
        out_specs=(P(None, "dom"), P("dom"), P("dom")),
        check_vma=False,
    )
```

```python
import functools

import jax
import jax.numpy as jnp
from jax import lax
from jax.experimental import pallas as pl
from jax.experimental.pallas import tpu as pltpu
from jax.sharding import PartitionSpec as P

LANES = 128
SUBS = 8
SUBSTEPS = 6
TEAM = 4
OFFSETS = (1, -1, 2, -2)
horizontal_rate = 0.5
vertical_rate = 0.5
tracer_step = 0.2
barotropic_step = 0.5
friction = 0.05
ABSENT = 3e38
PRESENT = 1e38

SMEM = pl.BlockSpec(memory_space=pltpu.SMEM)
VMEM = pl.BlockSpec(memory_space=pltpu.VMEM)
HBM = pl.BlockSpec(memory_space=pltpu.HBM)


def even_swap(count, by):
    return [(i, i ^ by) for i in range(count)]


def odd_swap(count, by):
    pairs = [(i, i + by) for i in range(by, count - by) if (i // by) % 2 == 1]
    pairs += [(b, a) for a, b in pairs]
    busy = {a for a, _ in pairs}
    rest = [i for i in range(count) if i not in busy]
    pairs += list(zip(rest[0::2], rest[1::2])) + list(zip(rest[1::2], rest[0::2]))
    return pairs


def column(scalars, tile):
    rows = lax.broadcasted_iota(jnp.int32, (SUBS, LANES), 0)
    value = jnp.zeros((SUBS, LANES), jnp.float32)
    for k in range(SUBS):
        value = jnp.where(rows == k, scalars[tile * SUBS + k], value)
    return value


def localize(index, place, count, cells, send):
    span = send * LANES
    result = index
    for g, offset in enumerate(OFFSETS):
        source = place - offset
        inside = jnp.logical_and(source >= 0, source < count)
        swapped = (place // abs(offset)) % 2 == 0
        step = jnp.where(swapped, span if g % 2 == 0 else -span, 0)
        low = cells + g * span
        mine = jnp.logical_and(index >= low, index < low + span)
        moved = jnp.where(inside, index + step, cells + 4 * span)
        result = jnp.where(mine, moved, result)
    return result


def group_of(rows, send):
    return rows // send


def blend(rows, send, parts):
    value = jnp.zeros((SUBS, LANES), jnp.float32)
    for g, part in parts.items():
        value = jnp.where(group_of(rows, send) == g, part, value)
    return value


def outgoing(field, slots):
    taken = jnp.take_along_axis(field, jnp.maximum(slots, 0), axis=0)
    return jnp.where(slots >= 0, taken, 0.0)


def prepare(
    place_ref, slots, thick, tracer_hbm, bottom_hbm, index_hbm, weight_hbm, ssh_hbm, velocity_hbm,
    near, side, far, odd, odd_side, tracer, bottom, index, weight, ssh, velocity, sems,
    *, count, send,
):
    sources = (bottom_hbm, tracer_hbm, index_hbm, weight_hbm, ssh_hbm, velocity_hbm)
    targets = (bottom, tracer, index, weight, ssh, velocity)
    copies = [
        pltpu.make_async_copy(source, target, sems.at[n])
        for n, (source, target) in enumerate(zip(sources, targets))
    ]
    for copy in copies:
        copy.start()
    levels, cells = tracer.shape
    tiles = levels // SUBS
    blocks = cells // LANES
    edges = index.shape[0]
    rows = lax.broadcasted_iota(jnp.int32, (SUBS, LANES), 0)
    place = place_ref[0]
    copies[0].wait()
    copies[1].wait()
    for way, out in enumerate((near, odd, side, odd_side)):
        offset = 1 if way < 2 else 2
        first = (place // offset) % 2 == 0
        base = 0 if way < 2 else 2
        start = out.shape[0] - send * levels
        for slot in range(send):
            block = jnp.where(
                first, slots[0, slot, base + way % 2], slots[0, slot, base + 1 - way % 2]
            )
            safe = jnp.maximum(block, 0)
            depth = jnp.where(block >= 0, bottom[pl.ds(safe, 1), :], 0)
            at = pl.multiple_of(safe * LANES, LANES)
            for k in range(tiles):
                value = tracer[k * SUBS : (k + 1) * SUBS, pl.ds(at, LANES)]
                row = start + slot * levels + k * SUBS
                out[row : row + SUBS, :] = jnp.where(rows + k * SUBS < depth, value, ABSENT)
    for copy in copies[2:]:
        copy.wait()
    own_tables(place, slots, thick, tracer, bottom, index, weight, ssh, velocity, far, count, send)
    for k in range(far.shape[0] // SUBS):
        at = slice(k * SUBS, (k + 1) * SUBS)
        near[at, :] = far[at, :]
        side[at, :] = far[at, :]


def own_tables(
    place, slots, thick, tracer, bottom, index, weight, ssh, velocity, mine, count, send
):
    levels, cells = tracer.shape
    tiles = levels // SUBS
    blocks = cells // LANES
    edges = index.shape[0]
    rows = lax.broadcasted_iota(jnp.int32, (SUBS, LANES), 0)
    thicks = [column(thick, k) for k in range(tiles)]
    sent = jnp.zeros((SUBS, LANES), jnp.float32)
    for g in range(4):
        for slot in range(send):
            sent = jnp.where(rows == g * send + slot, slots[0, slot, g].astype(jnp.float32), sent)
    team = (2 * edges + 3) * SUBS
    mine[team : team + SUBS, :] = sent
    for b in range(blocks):
        top = jnp.zeros((SUBS, LANES), jnp.float32)
        low = jnp.zeros((SUBS, LANES), jnp.float32)
        depth = bottom[b : b + 1, :]
        for k in range(tiles):
            layer = jnp.where(rows + k * SUBS < depth, thicks[k], 0.0)
            top = top + layer * tracer[k * SUBS : (k + 1) * SUBS, b * LANES : (b + 1) * LANES]
            low = low + layer
        row = 2 * edges * SUBS + b
        mine[row : row + 1, :] = jnp.sum(top, axis=0, keepdims=True) / jnp.sum(
            low, axis=0, keepdims=True
        )
    for b in range(blocks):
        lanes = slice(b * LANES, (b + 1) * LANES)
        for j in range(edges):
            row = j * SUBS + b
            mine[row : row + 1, :] = index[j : j + 1, lanes].astype(jnp.float32)
            row = (edges + j) * SUBS + b
            mine[row : row + 1, :] = weight[j : j + 1, lanes]
    for j in range(edges):
        at = slice(j * SUBS, (j + 1) * SUBS)
        mine[at, :] = bounded(mine[at, :], place, count, cells, send)
    row = (2 * edges + 1) * SUBS
    mine[row : row + SUBS, :] = velocity[...]
    mine[row + SUBS : row + 2 * SUBS, :] = ssh[...]


def bounded(index, place, count, cells, send):
    span = send * LANES
    result = index
    for g, offset in enumerate(OFFSETS):
        source = place - offset
        inside = jnp.logical_and(source >= 0, source < count)
        low = jnp.where(inside, cells + 4 * span, cells + g * span)
        low = low.astype(index.dtype)
        mine = jnp.logical_and(index >= low, index < cells + (g + 1) * span)
        result = jnp.where(mine, jnp.asarray(cells + 4 * span, index.dtype), result)
    return result


def gathered(rows_of, index, weight, own, pairs):
    laplace = jnp.zeros_like(own)
    for j in range(len(index)):
        lane = jnp.bitwise_and(index[j], LANES - 1)
        block = jnp.right_shift(index[j], 7)
        got = jnp.zeros_like(own)
        for r in range(pairs):
            got = jnp.where(block == r, jnp.take_along_axis(rows_of(r), lane, axis=1), got)
        laplace = laplace + weight[j] * (got - own)
    return laplace


def stepped(laplace, forcing, own, speed):
    faster = (1.0 - friction) * speed + barotropic_step * (laplace + forcing)
    return own + barotropic_step * faster, faster


def pack_edges(heights, speeds, slots, rows, send, even, way_even, way_odd):
    out = [outgoing(h, s) for h, s in zip(heights, slots)]
    fast = [outgoing(v, slots[q]) for q, v in enumerate(speeds)]
    right = [
        heights[3],
        heights[2],
        blend(rows, send, {0: out[2], 2: out[1]}),
        blend(rows, send, {0: out[1], 1: out[3], 2: out[0]}),
        edge_rows(out[3], out[2], rows, send, True),
        edge_rows(fast[3], fast[2], rows, send, True),
    ]
    left = [
        heights[0],
        heights[1],
        blend(rows, send, {1: out[1], 3: out[2]}),
        blend(rows, send, {0: out[0], 1: out[2], 3: out[3]}),
        edge_rows(out[0], out[1], rows, send, False),
        edge_rows(fast[0], fast[1], rows, send, False),
    ]
    for k in range(len(right)):
        at = slice(k * SUBS, (k + 1) * SUBS)
        way_even[at, :] = jnp.where(even, right[k], left[k])
        way_odd[at, :] = jnp.where(even, left[k], right[k])


def edge_rows(inner, outer, rows, send, rightward):
    if rightward:
        return jnp.where(group_of(rows, send) == 3, pltpu.roll(outer, send, 0), inner)
    return jnp.where(group_of(rows, send) == 2, pltpu.roll(outer, SUBS - send, 0), inner)


def gather_team(
    place_ref, mine, near, side, far, index, weight, force, slots, height, speed, way_even, way_odd,
    *, send,
):
    edges = index.shape[1]
    place = place_ref[0]
    position = place % TEAM
    even = (place // TEAM) % 2 == 0
    rows = lax.broadcasted_iota(jnp.int32, (SUBS, LANES), 0)
    for flip, ref in enumerate((mine, near, side, far)):
        q = jnp.bitwise_xor(position, flip)
        for j in range(edges):
            index[q, j] = ref[j * SUBS : (j + 1) * SUBS, :].astype(jnp.int32)
            weight[q, j] = ref[(edges + j) * SUBS : (edges + j + 1) * SUBS, :]
        row = 2 * edges * SUBS
        force[q] = ref[row : row + SUBS, :]
        speed[q] = ref[row + SUBS : row + 2 * SUBS, :]
        height[q] = ref[row + 2 * SUBS : row + 3 * SUBS, :]
        slots[q] = ref[row + 3 * SUBS : row + 4 * SUBS, :].astype(jnp.int32)
    held = [slots[q] for q in range(TEAM)]
    pack_edges(
        [height[q] for q in range(TEAM)], [speed[q] for q in range(TEAM)], held, rows, send, even,
        way_even, way_odd,
    )

    def both(k, field):
        at = slice((6 + k) * SUBS, (7 + k) * SUBS)
        picked = [outgoing(field(q), held[q]) for q in range(TEAM)]
        right = edge_rows(picked[3], picked[2], rows, send, True)
        left = edge_rows(picked[0], picked[1], rows, send, False)
        way_even[at, :] = jnp.where(even, right, left)
        way_odd[at, :] = jnp.where(even, left, right)

    for j in range(edges):
        both(j, lambda q: index[q, j].astype(jnp.float32))
        both(edges + j, lambda q: weight[q, j])
    both(2 * edges, lambda q: force[q])


def double_step(
    place, index, weight, force, slots, height_in, speed_in, total_in, even_in, odd_in, first_even,
    first_odd, height, speed, total, ext, virtual, only, *, send,
):
    edges = index.shape[1]
    even = (place // TEAM) % 2 == 0
    rows = lax.broadcasted_iota(jnp.int32, (SUBS, LANES), 0)
    held = [slots[q] for q in range(TEAM)]

    def side_of(k, constant, right):
        ref_even, ref_odd = (first_even, first_odd) if constant else (even_in, odd_in)
        at = slice(k * SUBS, (k + 1) * SUBS)
        a, b = ref_even[at, :], ref_odd[at, :]
        return jnp.where(even, a, b) if right else jnp.where(even, b, a)

    def fill(heights, left, right):
        out = [outgoing(h, s) for h, s in zip(heights, held)]
        halos = (
            {0: left, 1: out[1], 2: pltpu.roll(left, SUBS - send, 0), 3: out[2]},
            {0: out[0], 1: out[2], 2: left, 3: out[3]},
            {0: out[1], 1: out[3], 2: out[0], 3: right},
            {0: out[2], 1: right, 2: out[1], 3: pltpu.roll(right, send, 0)},
        )
        for q in range(TEAM):
            ext[q, 0:SUBS, :] = heights[q]
            ext[q, SUBS : 2 * SUBS, :] = blend(rows, send, halos[q])
        return out

    def advance_team(heights, speeds):
        moved = []
        for q in range(TEAM):
            laplace = gathered(
                lambda r: jnp.broadcast_to(ext[q, r : r + 1, :], (SUBS, LANES)),
                [index[q, j] for j in range(edges)],
                [weight[q, j] for j in range(edges)],
                heights[q],
                2 * SUBS,
            )
            moved.append(stepped(laplace, force[q], heights[q], speeds[q]))
        return [m[0] for m in moved], [m[1] for m in moved]

    heights = [height_in[q] for q in range(TEAM)]
    speeds = [speed_in[q] for q in range(TEAM)]
    edge = [side_of(4, False, right) for right in (False, True)]
    out = fill(heights, edge[0], edge[1])
    virtual[0, 0:SUBS, :] = side_of(0, False, False)
    virtual[0, SUBS : 2 * SUBS, :] = side_of(2, False, False) + blend(
        rows, send, {1: out[0], 3: out[1]}
    )
    virtual[1, 0:SUBS, :] = side_of(1, False, False)
    virtual[1, SUBS : 2 * SUBS, :] = side_of(3, False, False) + blend(rows, send, {3: out[0]})
    virtual[2, 0:SUBS, :] = side_of(0, False, True)
    virtual[2, SUBS : 2 * SUBS, :] = side_of(2, False, True) + blend(
        rows, send, {0: out[3], 2: out[2]}
    )
    virtual[3, 0:SUBS, :] = side_of(1, False, True)
    virtual[3, SUBS : 2 * SUBS, :] = side_of(3, False, True) + blend(rows, send, {2: out[3]})
    later, faster = advance_team(heights, speeds)
    for number, right in enumerate((False, True)):
        moved_group = 2 if right else 3
        laplace = gathered(
            lambda r: jnp.where(
                group_of(rows, send) == moved_group,
                virtual[2 * number + 1, r : r + 1, :],
                virtual[2 * number, r : r + 1, :],
            ),
            [side_of(6 + j, True, right).astype(jnp.int32) for j in range(edges)],
            [side_of(6 + edges + j, True, right) for j in range(edges)],
            edge[number],
            2 * SUBS,
        )
        edge[number] = stepped(
            laplace, side_of(6 + 2 * edges, True, right), edge[number], side_of(5, False, right)
        )[0]
    fill(later, edge[0], edge[1])
    if only is not None:
        for q in range(TEAM):
            height[q] = later[q]
            speed[q] = faster[q]
        q = only
        laplace = gathered(
            lambda r: jnp.broadcast_to(ext[q, r : r + 1, :], (SUBS, LANES)),
            [index[q, j] for j in range(edges)],
            [weight[q, j] for j in range(edges)],
            height[q],
            2 * SUBS,
        )
        before = total_in[q] + speed[q]
        height[q], speed[q] = stepped(laplace, force[q], height[q], speed[q])
        total[q] = before + speed[q]
        return None
    last, fastest = advance_team(later, faster)
    for q in range(TEAM):
        height[q] = last[q]
        speed[q] = fastest[q]
        before = 0.0 if total_in is None else total_in[q]
        total[q] = before + faster[q] + fastest[q]
    return last, fastest, held, rows, even


def first_pair(
    place, index, weight, force, slots, height_in, speed_in, even_in, odd_in, height, speed, total,
    way_even, way_odd, ext, virtual, *, send,
):
    last, fastest, held, rows, even = double_step(
        place[0], index, weight, force, slots, height_in, speed_in, None, even_in, odd_in, even_in,
        odd_in, height, speed, total, ext, virtual, None, send=send,
    )
    pack_edges(last, fastest, held, rows, send, even, way_even, way_odd)


def middle_pair(
    place, index, weight, force, slots, height_in, speed_in, total_in, even_in, odd_in, first_even,
    first_odd, height, speed, total, way_even, way_odd, ext, virtual, *, send,
):
    last, fastest, held, rows, even = double_step(
        place[0], index, weight, force, slots, height_in, speed_in, total_in, even_in, odd_in,
        first_even, first_odd, height, speed, total, ext, virtual, None, send=send,
    )
    pack_edges(last, fastest, held, rows, send, even, way_even, way_odd)


def last_pair(
    place_ref, index, weight, force, slots, height_in, speed_in, total_in, even_in, odd_in,
    first_even, first_odd, bottom, base, shape, new_height, new_speed, out_hbm, out, height, speed,
    total, ext, virtual, sems, *, send,
):
    position = place_ref[0] % TEAM
    double_step(
        place_ref[0], index, weight, force, slots, height_in, speed_in, total_in, even_in, odd_in,
        first_even, first_odd, height, speed, total, ext, virtual, position, send=send,
    )
    new_height[...] = height[position]
    new_speed[...] = speed[position]
    ext[0, 0:SUBS, :] = total[position] / SUBSTEPS
    rows = lax.broadcasted_iota(jnp.int32, (SUBS, LANES), 0)
    copies = []
    for k in range(out.shape[0] // SUBS):
        levels = slice(k * SUBS, (k + 1) * SUBS)
        for i in range(out.shape[1] // LANES):
            at = (levels, slice(i * LANES, (i + 1) * LANES))
            added = jnp.where(rows + k * SUBS < bottom[i : i + 1, :], shape[levels, :], 0.0)
            out[at] = base[at] + added * ext[0, i : i + 1, :]
        copies.append(
            pltpu.make_async_copy(out.at[levels, :], out_hbm.at[levels, :], sems.at[k])
        )
        copies[-1].start()
    for copy in copies:
        copy.wait()


def collected(sources, index, weight, mine, tiles):
    flat = [jnp.zeros((SUBS, LANES), jnp.float32) for _ in range(tiles)]
    for near, factor in zip(index, weight):
        near = jnp.broadcast_to(near, (SUBS, LANES))
        lane = jnp.bitwise_and(near, LANES - 1)
        block = jnp.right_shift(near, 7)
        got = [jnp.full((SUBS, LANES), ABSENT, jnp.float32) for _ in range(tiles)]
        for r, source in sources:
            here = block == r
            for k in range(tiles):
                found = jnp.take_along_axis(source(k), lane, axis=1)
                got[k] = jnp.where(here, found, got[k])
        for k in range(tiles):
            flat[k] = flat[k] + factor * jnp.where(got[k] < PRESENT, got[k] - mine[k], 0.0)
    return flat


def tracer_own(
    place_ref, slots, thick, profile, tracer, bottom, index, weight, ssh, velocity, out, shape, mine_out,
    held, *, count, send,
):
    own_tables(
        place_ref[0], slots, thick, tracer, bottom, index, weight, ssh, velocity, mine_out, count, send
    )
    levels, cells = tracer.shape
    tiles = levels // SUBS
    blocks = cells // LANES
    edges = index.shape[0]
    rows = lax.broadcasted_iota(jnp.int32, (SUBS, LANES), 0)
    for i in range(blocks):
        depth = bottom[i : i + 1, :]
        for k in range(tiles):
            at = (slice(k * SUBS, (k + 1) * SUBS), slice(i * LANES, (i + 1) * LANES))
            held[at] = jnp.where(rows + k * SUBS < depth, tracer[at], ABSENT)
    for k in range(tiles):
        shape[k * SUBS : (k + 1) * SUBS, :] = column(profile, k)

    def source(r):
        return lambda k: held[k * SUBS : (k + 1) * SUBS, r * LANES : (r + 1) * LANES]

    def cell_block(i, carry):
        lanes = pl.ds(pl.multiple_of(i * LANES, LANES), LANES)
        depth = bottom[pl.ds(i, 1), :]
        mine = [tracer[k * SUBS : (k + 1) * SUBS, lanes] for k in range(tiles)]
        flat = collected(
            [(r, source(r)) for r in range(blocks)],
            [index[j : j + 1, lanes] for j in range(edges)],
            [weight[j : j + 1, lanes] for j in range(edges)],
            mine,
            tiles,
        )
        for k in range(tiles):
            first = rows + k * SUBS
            value = mine[k]
            up = pltpu.roll(value, SUBS - 1, 0)
            if k + 1 < tiles:
                up = jnp.where(rows == SUBS - 1, pltpu.roll(mine[k + 1], SUBS - 1, 0), up)
            down = pltpu.roll(value, 1, 0)
            if k > 0:
                down = jnp.where(rows == 0, pltpu.roll(mine[k - 1], 1, 0), down)
            below = jnp.where(first + 1 < jnp.minimum(depth, levels), up - value, 0.0)
            above = jnp.where(first > 0, down - value, 0.0)
            moved = horizontal_rate * flat[k] + vertical_rate * (below + above)
            out[k * SUBS : (k + 1) * SUBS, lanes] = value + tracer_step * jnp.where(
                first < depth, moved, 0.0
            )
        return carry

    lax.fori_loop(0, blocks, cell_block, 0)


def tracer_halo(place_ref, tracer, bottom, index, weight, part, a, b, c, d, out, *, count, send):
    levels, cells = tracer.shape
    tiles = levels // SUBS
    blocks = cells // LANES
    edges = index.shape[0]
    arrived = (a, b, c, d)
    rows = lax.broadcasted_iota(jnp.int32, (SUBS, LANES), 0)
    place = place_ref[0]

    def source(r):
        ref = arrived[r // send]
        start = ref.shape[0] - send * levels + r % send * levels
        return lambda k: ref[start + k * SUBS : start + (k + 1) * SUBS, :]

    def cell_block(i, carry):
        lanes = pl.ds(pl.multiple_of(i * LANES, LANES), LANES)
        depth = bottom[pl.ds(i, 1), :]
        mine = [tracer[k * SUBS : (k + 1) * SUBS, lanes] for k in range(tiles)]
        flat = collected(
            [(blocks + r, source(r)) for r in range(4 * send)],
            [
                localize(index[j : j + 1, lanes], place, count, cells, send)
                for j in range(edges)
            ],
            [weight[j : j + 1, lanes] for j in range(edges)],
            mine,
            tiles,
        )
        for k in range(tiles):
            at = (slice(k * SUBS, (k + 1) * SUBS), lanes)
            added = jnp.where(rows + k * SUBS < depth, horizontal_rate * flat[k], 0.0)
            out[at] = part[at] + tracer_step * added
        return carry

    lax.fori_loop(0, blocks, cell_block, 0)


def shards(
    tracer, bottom_levels, neighbours, edge_weight, ssh, velocity, send_blocks, thickness, profile
):
    count = lax.axis_size("dom")
    levels, cells = tracer.shape
    send = send_blocks.shape[-1]
    edges = neighbours.shape[0]
    blocks = cells // LANES
    assert blocks == SUBS and 4 * send == SUBS and levels % SUBS == 0 and count % (2 * TEAM) == 0
    assert SUBSTEPS == 6
    tile = (blocks, LANES)
    place = lax.axis_index("dom").astype(jnp.int32)[None]
    slots = jnp.swapaxes(send_blocks, 1, 2)
    bottom = bottom_levels.reshape(tile)

    def shape(rows, kind=jnp.float32):
        return jax.ShapeDtypeStruct(rows, kind)

    def call(body, name, outs, ins, scratch, flops, limit=4):
        return pl.pallas_call(
            functools.partial(body, send=send),
            out_shape=outs,
            in_specs=ins,
            scratch_shapes=scratch,
            compiler_params=pltpu.CompilerParams(vmem_limit_bytes=limit << 20),
            cost_estimate=pl.CostEstimate(flops=flops, bytes_accessed=1000, transcendentals=0),
            name=name,
        )

    own = (2 * edges + 4) * SUBS
    halo = send * levels
    near, side, far, odd, odd_side = call(
        functools.partial(prepare, count=count),
        "prepare",
        [
            shape((own + halo, LANES)),
            shape((own + halo, LANES)),
            shape((own, LANES)),
            shape((halo, LANES)),
            shape((halo, LANES)),
        ],
        [SMEM, SMEM, SMEM] + [HBM] * 6,
        [
            pltpu.VMEM(tracer.shape, jnp.float32),
            pltpu.VMEM(tile, jnp.int32),
            pltpu.VMEM(neighbours.shape, jnp.int32),
            pltpu.VMEM(edge_weight.shape, jnp.float32),
            pltpu.VMEM(tile, jnp.float32),
            pltpu.VMEM(tile, jnp.float32),
            pltpu.SemaphoreType.DMA((6,)),
        ],
        4000000,
        60,
    )(
        place, slots, thickness, tracer, bottom, neighbours, edge_weight, ssh.reshape(tile),
        velocity.reshape(tile),
    )
    part, columns, mine = call(
        functools.partial(tracer_own, count=count),
        "tracer_own",
        [shape(tracer.shape), shape((levels, LANES)), shape((own, LANES))],
        [SMEM] * 4 + [VMEM] * 6,
        [pltpu.VMEM(tracer.shape, jnp.float32)],
        10000000,
    )(
        place, slots, thickness, profile, tracer, bottom, neighbours, edge_weight,
        ssh.reshape(tile), velocity.reshape(tile),
    )
    side = lax.ppermute(side, "dom", even_swap(count, 2))
    far = lax.ppermute(far, "dom", even_swap(count, 3))
    near = lax.ppermute(near, "dom", even_swap(count, 1))
    odd = lax.ppermute(odd, "dom", odd_swap(count, 1))
    odd_side = lax.ppermute(odd_side, "dom", odd_swap(count, 2))

    def swap(pair):
        return (
            lax.ppermute(pair[0], "dom", even_swap(count, TEAM)),
            lax.ppermute(pair[1], "dom", odd_swap(count, TEAM)),
        )

    state = [shape((TEAM,) + tile)] * 2
    entire = (6 + 2 * edges + 1) * SUBS
    *tables, height, speed, way_even, way_odd = call(
        gather_team,
        "gather_team",
        [
            shape((TEAM, edges) + tile, jnp.int32),
            shape((TEAM, edges) + tile),
            shape((TEAM,) + tile),
            shape((TEAM,) + tile, jnp.int32),
        ]
        + state
        + [shape((entire, LANES))] * 2,
        [SMEM] + [VMEM] * 4,
        [],
        500000,
    )(place, mine, near, side, far)
    constant = swap((way_even, way_odd))
    base = call(
        functools.partial(tracer_halo, count=count),
        "tracer_halo",
        shape(tracer.shape),
        [SMEM] + [VMEM] * 9,
        [],
        10000000,
    )(place, tracer, bottom, neighbours, edge_weight, part, near, odd, side, odd_side)
    scratch = [pltpu.VMEM((TEAM, 2 * SUBS, LANES), jnp.float32)] * 2
    light = [shape((6 * SUBS, LANES))] * 2
    height, speed, total, *ways = call(
        first_pair, "first_pair", state + state[:1] + light, [SMEM] + [VMEM] * 8, scratch, 2000000
    )(place, *tables, height, speed, *constant)
    arrived = swap(ways)
    height, speed, total, *ways = call(
        middle_pair, "middle_pair", state + state[:1] + light, [SMEM] + [VMEM] * 11, scratch, 2000000
    )(place, *tables, height, speed, total, *arrived, *constant)
    arrived = swap(ways)
    team_scratch = [pltpu.VMEM((TEAM,) + tile, jnp.float32)] * 3
    height, speed, result = pl.pallas_call(
        functools.partial(last_pair, send=send),
        out_shape=[shape(tile), shape(tile), shape(tracer.shape)],
        in_specs=[SMEM] + [VMEM] * 14,
        out_specs=[VMEM, VMEM, HBM],
        scratch_shapes=[pltpu.VMEM(tracer.shape, jnp.float32)]
        + team_scratch
        + scratch
        + [pltpu.SemaphoreType.DMA((levels // SUBS,))],
        compiler_params=pltpu.CompilerParams(vmem_limit_bytes=4 << 20),
        cost_estimate=pl.CostEstimate(flops=2500000, bytes_accessed=1000, transcendentals=0),
        name="last_pair",
    )(place, *tables, height, speed, total, *arrived, *constant, bottom, base, columns)
    return (result, height.reshape(-1), speed.reshape(-1))


def solution(mesh):
    placed = (
        P(None, "dom"),
        P("dom"),
        P(None, "dom"),
        P(None, "dom"),
        P("dom"),
        P("dom"),
        P("dom", None, None),
        P(),
        P(),
    )
    return jax.shard_map(
        shards,
        mesh=mesh,
        in_specs=placed,
        out_specs=(P(None, "dom"), P("dom"), P("dom")),
        check_vma=False,
    )
```

```python
import functools

import jax
import jax.numpy as jnp
from jax import lax
from jax.experimental import pallas as pl
from jax.experimental.pallas import tpu as pltpu
from jax.sharding import PartitionSpec as P


LANES = 128
SUBS = 8
SUBSTEPS = 6
TEAM = 4
OFFSETS = (1, -1, 2, -2)
horizontal_rate = 0.5
vertical_rate = 0.5
tracer_step = 0.2
barotropic_step = 0.5
friction = 0.05
ABSENT = 3e38
PRESENT = 1e38


SMEM = pl.BlockSpec(memory_space=pltpu.SMEM)
VMEM = pl.BlockSpec(memory_space=pltpu.VMEM)
HBM = pl.BlockSpec(memory_space=pltpu.HBM)


def even_swap(count, by):
    return [(i, i ^ by) for i in range(count)]


def odd_swap(count, by):
    pairs = [(i, i + by) for i in range(by, count - by) if (i // by) % 2 == 1]
    pairs += [(b, a) for a, b in pairs]
    busy = {a for a, _ in pairs}
    rest = [i for i in range(count) if i not in busy]
    pairs += list(zip(rest[0::2], rest[1::2])) + list(zip(rest[1::2], rest[0::2]))
    return pairs


def column(scalars, tile):
    rows = lax.broadcasted_iota(jnp.int32, (SUBS, LANES), 0)
    value = jnp.zeros((SUBS, LANES), jnp.float32)
    for k in range(SUBS):
        value = jnp.where(rows == k, scalars[tile * SUBS + k], value)
    return value


def localize(index, place, count, cells, send):
    span = send * LANES
    result = index
    for g, offset in enumerate(OFFSETS):
        source = place - offset
        inside = jnp.logical_and(source >= 0, source < count)
        swapped = (place // abs(offset)) % 2 == 0
        step = jnp.where(swapped, span if g % 2 == 0 else -span, 0)
        low = cells + g * span
        mine = jnp.logical_and(index >= low, index < low + span)
        moved = jnp.where(inside, index + step, cells + 4 * span)
        result = jnp.where(mine, moved, result)
    return result


def group_of(rows, send):
    return rows // send


def blend(rows, send, parts):
    value = jnp.zeros((SUBS, LANES), jnp.float32)
    for g, part in parts.items():
        value = jnp.where(group_of(rows, send) == g, part, value)
    return value


def outgoing(field, slots):
    taken = jnp.take_along_axis(field, jnp.maximum(slots, 0), axis=0)
    return jnp.where(slots >= 0, taken, 0.0)


def tracer_blocks(place, slots, tracer, bottom, outs, send):
    levels = tracer.shape[0]
    tiles = levels // SUBS
    rows = lax.broadcasted_iota(jnp.int32, (SUBS, LANES), 0)
    for way, out in outs:
        offset = 1 if way < 2 else 2
        first = (place // offset) % 2 == 0
        base = 0 if way < 2 else 2
        start = out.shape[0] - send * levels
        for slot in range(send):
            block = jnp.where(
                first, slots[0, slot, base + way % 2], slots[0, slot, base + 1 - way % 2]
            )
            safe = jnp.maximum(block, 0)
            depth = jnp.where(block >= 0, bottom[pl.ds(safe, 1), :], 0)
            at = pl.multiple_of(safe * LANES, LANES)
            for k in range(tiles):
                value = tracer[k * SUBS : (k + 1) * SUBS, pl.ds(at, LANES)]
                row = start + slot * levels + k * SUBS
                out[row : row + SUBS, :] = jnp.where(rows + k * SUBS < depth, value, ABSENT)


def prepare(
    place_ref, slots, thick, tracer, bottom, index, weight, ssh, velocity, near, side, far, *,
    count, send,
):
    place = place_ref[0]
    tracer_blocks(place, slots, tracer, bottom, ((0, near), (2, side)), send)
    own_tables(place, slots, thick, tracer, bottom, index, weight, ssh, velocity, far, count, send)
    for k in range(far.shape[0] // SUBS):
        at = slice(k * SUBS, (k + 1) * SUBS)
        near[at, :] = far[at, :]
        side[at, :] = far[at, :]


def own_tables(
    place, slots, thick, tracer, bottom, index, weight, ssh, velocity, mine, count, send
):
    levels, cells = tracer.shape
    tiles = levels // SUBS
    blocks = cells // LANES
    edges = index.shape[0]
    rows = lax.broadcasted_iota(jnp.int32, (SUBS, LANES), 0)
    thicks = [column(thick, k) for k in range(tiles)]
    sent = jnp.zeros((SUBS, LANES), jnp.float32)
    for g in range(4):
        for slot in range(send):
            sent = jnp.where(rows == g * send + slot, slots[0, slot, g].astype(jnp.float32), sent)
    team = (2 * edges + 3) * SUBS
    mine[team : team + SUBS, :] = sent
    for b in range(blocks):
        top = jnp.zeros((SUBS, LANES), jnp.float32)
        low = jnp.zeros((SUBS, LANES), jnp.float32)
        depth = bottom[b : b + 1, :]
        for k in range(tiles):
            layer = jnp.where(rows + k * SUBS < depth, thicks[k], 0.0)
            top = top + layer * tracer[k * SUBS : (k + 1) * SUBS, b * LANES : (b + 1) * LANES]
            low = low + layer
        row = 2 * edges * SUBS + b
        mine[row : row + 1, :] = jnp.sum(top, axis=0, keepdims=True) / jnp.sum(
            low, axis=0, keepdims=True
        )
    for b in range(blocks):
        lanes = slice(b * LANES, (b + 1) * LANES)
        for j in range(edges):
            row = j * SUBS + b
            mine[row : row + 1, :] = index[j : j + 1, lanes].astype(jnp.float32)
            row = (edges + j) * SUBS + b
            mine[row : row + 1, :] = weight[j : j + 1, lanes]
    for j in range(edges):
        at = slice(j * SUBS, (j + 1) * SUBS)
        mine[at, :] = bounded(mine[at, :], place, count, cells, send)
    row = (2 * edges + 1) * SUBS
    mine[row : row + SUBS, :] = velocity[...]
    mine[row + SUBS : row + 2 * SUBS, :] = ssh[...]


def bounded(index, place, count, cells, send):
    span = send * LANES
    result = index
    for g, offset in enumerate(OFFSETS):
        source = place - offset
        inside = jnp.logical_and(source >= 0, source < count)
        low = jnp.where(inside, cells + 4 * span, cells + g * span)
        low = low.astype(index.dtype)
        mine = jnp.logical_and(index >= low, index < cells + (g + 1) * span)
        result = jnp.where(mine, jnp.asarray(cells + 4 * span, index.dtype), result)
    return result


def gathered(rows_of, index, weight, own, pairs):
    laplace = jnp.zeros_like(own)
    for j in range(len(index)):
        lane = jnp.bitwise_and(index[j], LANES - 1)
        block = jnp.right_shift(index[j], 7)
        got = jnp.zeros_like(own)
        for r in range(pairs):
            got = jnp.where(block == r, jnp.take_along_axis(rows_of(r), lane, axis=1), got)
        laplace = laplace + weight[j] * (got - own)
    return laplace


def stepped(laplace, forcing, own, speed):
    faster = (1.0 - friction) * speed + barotropic_step * (laplace + forcing)
    return own + barotropic_step * faster, faster


def pack_edges(heights, speeds, slots, rows, send, even, way_even, way_odd):
    out = [outgoing(h, s) for h, s in zip(heights, slots)]
    fast = [outgoing(v, slots[q]) for q, v in enumerate(speeds)]
    right = [
        heights[3],
        heights[2],
        blend(rows, send, {0: out[2], 2: out[1]}),
        blend(rows, send, {0: out[1], 1: out[3], 2: out[0]}),
        edge_rows(out[3], out[2], rows, send, True),
        edge_rows(fast[3], fast[2], rows, send, True),
    ]
    left = [
        heights[0],
        heights[1],
        blend(rows, send, {1: out[1], 3: out[2]}),
        blend(rows, send, {0: out[0], 1: out[2], 3: out[3]}),
        edge_rows(out[0], out[1], rows, send, False),
        edge_rows(fast[0], fast[1], rows, send, False),
    ]
    for k in range(len(right)):
        at = slice(k * SUBS, (k + 1) * SUBS)
        way_even[at, :] = jnp.where(even, right[k], left[k])
        way_odd[at, :] = jnp.where(even, left[k], right[k])


def edge_rows(inner, outer, rows, send, rightward):
    if rightward:
        return jnp.where(group_of(rows, send) == 3, pltpu.roll(outer, send, 0), inner)
    return jnp.where(group_of(rows, send) == 2, pltpu.roll(outer, SUBS - send, 0), inner)


def gather_team(
    place_ref, mine, near, side, far, index, weight, force, slots, height, speed, way_even, way_odd,
    *, send,
):
    edges = index.shape[1]
    place = place_ref[0]
    position = place % TEAM
    even = (place // TEAM) % 2 == 0
    rows = lax.broadcasted_iota(jnp.int32, (SUBS, LANES), 0)
    for flip, ref in enumerate((mine, near, side, far)):
        q = jnp.bitwise_xor(position, flip)
        for j in range(edges):
            index[q, j] = ref[j * SUBS : (j + 1) * SUBS, :].astype(jnp.int32)
            weight[q, j] = ref[(edges + j) * SUBS : (edges + j + 1) * SUBS, :]
        row = 2 * edges * SUBS
        force[q] = ref[row : row + SUBS, :]
        speed[q] = ref[row + SUBS : row + 2 * SUBS, :]
        height[q] = ref[row + 2 * SUBS : row + 3 * SUBS, :]
        slots[q] = ref[row + 3 * SUBS : row + 4 * SUBS, :].astype(jnp.int32)
    held = [slots[q] for q in range(TEAM)]
    pack_edges(
        [height[q] for q in range(TEAM)], [speed[q] for q in range(TEAM)], held, rows, send, even,
        way_even, way_odd,
    )

    def both(k, field):
        at = slice((6 + k) * SUBS, (7 + k) * SUBS)
        picked = [outgoing(field(q), held[q]) for q in range(TEAM)]
        right = edge_rows(picked[3], picked[2], rows, send, True)
        left = edge_rows(picked[0], picked[1], rows, send, False)
        way_even[at, :] = jnp.where(even, right, left)
        way_odd[at, :] = jnp.where(even, left, right)

    for j in range(edges):
        both(j, lambda q: index[q, j].astype(jnp.float32))
        both(edges + j, lambda q: weight[q, j])
    both(2 * edges, lambda q: force[q])


def double_step(
    place, index, weight, force, slots, height_in, speed_in, total_in, even_in, odd_in, first_even,
    first_odd, height, speed, total, ext, virtual, only, *, send,
):
    edges = index.shape[1]
    even = (place // TEAM) % 2 == 0
    rows = lax.broadcasted_iota(jnp.int32, (SUBS, LANES), 0)
    held = [slots[q] for q in range(TEAM)]

    def side_of(k, constant, right):
        ref_even, ref_odd = (first_even, first_odd) if constant else (even_in, odd_in)
        at = slice(k * SUBS, (k + 1) * SUBS)
        a, b = ref_even[at, :], ref_odd[at, :]
        return jnp.where(even, a, b) if right else jnp.where(even, b, a)

    def fill(heights, left, right):
        out = [outgoing(h, s) for h, s in zip(heights, held)]
        halos = (
            {0: left, 1: out[1], 2: pltpu.roll(left, SUBS - send, 0), 3: out[2]},
            {0: out[0], 1: out[2], 2: left, 3: out[3]},
            {0: out[1], 1: out[3], 2: out[0], 3: right},
            {0: out[2], 1: right, 2: out[1], 3: pltpu.roll(right, send, 0)},
        )
        for q in range(TEAM):
            ext[q, 0:SUBS, :] = heights[q]
            ext[q, SUBS : 2 * SUBS, :] = blend(rows, send, halos[q])
        return out

    def advance_team(heights, speeds):
        moved = []
        for q in range(TEAM):
            laplace = gathered(
                lambda r: jnp.broadcast_to(ext[q, r : r + 1, :], (SUBS, LANES)),
                [index[q, j] for j in range(edges)],
                [weight[q, j] for j in range(edges)],
                heights[q],
                2 * SUBS,
            )
            moved.append(stepped(laplace, force[q], heights[q], speeds[q]))
        return [m[0] for m in moved], [m[1] for m in moved]

    heights = [height_in[q] for q in range(TEAM)]
    speeds = [speed_in[q] for q in range(TEAM)]
    edge = [side_of(4, False, right) for right in (False, True)]
    out = fill(heights, edge[0], edge[1])
    virtual[0, 0:SUBS, :] = side_of(0, False, False)
    virtual[0, SUBS : 2 * SUBS, :] = side_of(2, False, False) + blend(
        rows, send, {1: out[0], 3: out[1]}
    )
    virtual[1, 0:SUBS, :] = side_of(1, False, False)
    virtual[1, SUBS : 2 * SUBS, :] = side_of(3, False, False) + blend(rows, send, {3: out[0]})
    virtual[2, 0:SUBS, :] = side_of(0, False, True)
    virtual[2, SUBS : 2 * SUBS, :] = side_of(2, False, True) + blend(
        rows, send, {0: out[3], 2: out[2]}
    )
    virtual[3, 0:SUBS, :] = side_of(1, False, True)
    virtual[3, SUBS : 2 * SUBS, :] = side_of(3, False, True) + blend(rows, send, {2: out[3]})
    later, faster = advance_team(heights, speeds)
    for number, right in enumerate((False, True)):
        moved_group = 2 if right else 3
        laplace = gathered(
            lambda r: jnp.where(
                group_of(rows, send) == moved_group,
                virtual[2 * number + 1, r : r + 1, :],
                virtual[2 * number, r : r + 1, :],
            ),
            [side_of(6 + j, True, right).astype(jnp.int32) for j in range(edges)],
            [side_of(6 + edges + j, True, right) for j in range(edges)],
            edge[number],
            2 * SUBS,
        )
        edge[number] = stepped(
            laplace, side_of(6 + 2 * edges, True, right), edge[number], side_of(5, False, right)
        )[0]
    fill(later, edge[0], edge[1])
    if only is not None:
        for q in range(TEAM):
            height[q] = later[q]
            speed[q] = faster[q]
        q = only
        laplace = gathered(
            lambda r: jnp.broadcast_to(ext[q, r : r + 1, :], (SUBS, LANES)),
            [index[q, j] for j in range(edges)],
            [weight[q, j] for j in range(edges)],
            height[q],
            2 * SUBS,
        )
        before = total_in[q] + speed[q]
        height[q], speed[q] = stepped(laplace, force[q], height[q], speed[q])
        total[q] = before + speed[q]
        return None
    last, fastest = advance_team(later, faster)
    for q in range(TEAM):
        height[q] = last[q]
        speed[q] = fastest[q]
        before = 0.0 if total_in is None else total_in[q]
        total[q] = before + faster[q] + fastest[q]
    return last, fastest, held, rows, even


def first_pair(
    place, index, weight, force, slots, height_in, speed_in, even_in, odd_in, height, speed, total,
    way_even, way_odd, ext, virtual, *, send,
):
    last, fastest, held, rows, even = double_step(
        place[0], index, weight, force, slots, height_in, speed_in, None, even_in, odd_in, even_in,
        odd_in, height, speed, total, ext, virtual, None, send=send,
    )
    pack_edges(last, fastest, held, rows, send, even, way_even, way_odd)


def middle_pair(
    place, index, weight, force, slots, height_in, speed_in, total_in, even_in, odd_in, first_even,
    first_odd, height, speed, total, way_even, way_odd, ext, virtual, *, send,
):
    last, fastest, held, rows, even = double_step(
        place[0], index, weight, force, slots, height_in, speed_in, total_in, even_in, odd_in,
        first_even, first_odd, height, speed, total, ext, virtual, None, send=send,
    )
    pack_edges(last, fastest, held, rows, send, even, way_even, way_odd)


def last_pair(
    place_ref, index, weight, force, slots, height_in, speed_in, total_in, even_in, odd_in,
    first_even, first_odd, bottom, base, shape, height_hbm, speed_hbm, out_hbm, out, height, speed,
    total, ext, virtual, sems, *, send,
):
    position = place_ref[0] % TEAM
    double_step(
        place_ref[0], index, weight, force, slots, height_in, speed_in, total_in, even_in, odd_in,
        first_even, first_odd, height, speed, total, ext, virtual, position, send=send,
    )
    ext[0, 0:SUBS, :] = total[position] / SUBSTEPS
    rows = lax.broadcasted_iota(jnp.int32, (SUBS, LANES), 0)
    tiles = out.shape[0] // SUBS
    copies = [
        pltpu.make_async_copy(height.at[position], height_hbm, sems.at[tiles]),
        pltpu.make_async_copy(speed.at[position], speed_hbm, sems.at[tiles + 1]),
    ]
    for copy in copies:
        copy.start()
    for k in range(out.shape[0] // SUBS):
        levels = slice(k * SUBS, (k + 1) * SUBS)
        for i in range(out.shape[1] // LANES):
            at = (levels, slice(i * LANES, (i + 1) * LANES))
            added = jnp.where(rows + k * SUBS < bottom[i : i + 1, :], shape[levels, :], 0.0)
            out[at] = base[at] + added * ext[0, i : i + 1, :]
        copies.append(
            pltpu.make_async_copy(out.at[levels, :], out_hbm.at[levels, :], sems.at[k])
        )
        copies[-1].start()
    for copy in copies:
        copy.wait()


def collected(sources, index, weight, mine, tiles):
    flat = [jnp.zeros((SUBS, LANES), jnp.float32) for _ in range(tiles)]
    for near, factor in zip(index, weight):
        near = jnp.broadcast_to(near, (SUBS, LANES))
        lane = jnp.bitwise_and(near, LANES - 1)
        block = jnp.right_shift(near, 7)
        got = [jnp.full((SUBS, LANES), ABSENT, jnp.float32) for _ in range(tiles)]
        for r, source in sources:
            here = block == r
            for k in range(tiles):
                found = jnp.take_along_axis(source(k), lane, axis=1)
                got[k] = jnp.where(here, found, got[k])
        for k in range(tiles):
            flat[k] = flat[k] + factor * jnp.where(got[k] < PRESENT, got[k] - mine[k], 0.0)
    return flat


def tracer_own(
    place_ref, slots, thick, profile, tracer, bottom, index, weight, ssh, velocity, out, shape, mine_out,
    odd, odd_side, local, held, *, count, send,
):
    own_tables(
        place_ref[0], slots, thick, tracer, bottom, index, weight, ssh, velocity, mine_out, count, send
    )
    tracer_blocks(place_ref[0], slots, tracer, bottom, ((1, odd), (3, odd_side)), send)
    for i in range(index.shape[1] // LANES):
        at = slice(i * LANES, (i + 1) * LANES)
        local[:, at] = localize(index[:, at], place_ref[0], count, index.shape[1], send)
    levels, cells = tracer.shape
    tiles = levels // SUBS
    blocks = cells // LANES
    edges = index.shape[0]
    rows = lax.broadcasted_iota(jnp.int32, (SUBS, LANES), 0)
    for i in range(blocks):
        depth = bottom[i : i + 1, :]
        for k in range(tiles):
            at = (slice(k * SUBS, (k + 1) * SUBS), slice(i * LANES, (i + 1) * LANES))
            held[at] = jnp.where(rows + k * SUBS < depth, tracer[at], ABSENT)
    for k in range(tiles):
        shape[k * SUBS : (k + 1) * SUBS, :] = column(profile, k)

    def source(r):
        return lambda k: held[k * SUBS : (k + 1) * SUBS, r * LANES : (r + 1) * LANES]

    def cell_block(i, carry):
        lanes = pl.ds(pl.multiple_of(i * LANES, LANES), LANES)
        depth = bottom[pl.ds(i, 1), :]
        mine = [tracer[k * SUBS : (k + 1) * SUBS, lanes] for k in range(tiles)]
        flat = collected(
            [(r, source(r)) for r in range(blocks)],
            [index[j : j + 1, lanes] for j in range(edges)],
            [weight[j : j + 1, lanes] for j in range(edges)],
            mine,
            tiles,
        )
        for k in range(tiles):
            first = rows + k * SUBS
            value = mine[k]
            up = pltpu.roll(value, SUBS - 1, 0)
            if k + 1 < tiles:
                up = jnp.where(rows == SUBS - 1, pltpu.roll(mine[k + 1], SUBS - 1, 0), up)
            down = pltpu.roll(value, 1, 0)
            if k > 0:
                down = jnp.where(rows == 0, pltpu.roll(mine[k - 1], 1, 0), down)
            below = jnp.where(first + 1 < jnp.minimum(depth, levels), up - value, 0.0)
            above = jnp.where(first > 0, down - value, 0.0)
            moved = horizontal_rate * flat[k] + vertical_rate * (below + above)
            out[k * SUBS : (k + 1) * SUBS, lanes] = value + tracer_step * jnp.where(
                first < depth, moved, 0.0
            )
        return carry

    lax.fori_loop(0, blocks, cell_block, 0)


def tracer_halo(tracer, bottom, local, weight, part, a, b, out, *, send, ways):
    levels, cells = tracer.shape
    tiles = levels // SUBS
    blocks = cells // LANES
    edges = local.shape[0]
    rows = lax.broadcasted_iota(jnp.int32, (SUBS, LANES), 0)

    def source(ref, slot):
        start = ref.shape[0] - send * levels + slot * levels
        return lambda k: ref[start + k * SUBS : start + (k + 1) * SUBS, :]

    sources = [
        (blocks + way * send + slot, source(ref, slot))
        for way, ref in zip(ways, (a, b))
        for slot in range(send)
    ]

    def cell_block(i, carry):
        lanes = pl.ds(pl.multiple_of(i * LANES, LANES), LANES)
        depth = bottom[pl.ds(i, 1), :]
        mine = [tracer[k * SUBS : (k + 1) * SUBS, lanes] for k in range(tiles)]
        near = [local[j : j + 1, lanes] for j in range(edges)]
        factors = [weight[j : j + 1, lanes] for j in range(edges)]
        flat = collected(sources, near, factors, mine, tiles)
        for k in range(tiles):
            at = (slice(k * SUBS, (k + 1) * SUBS), lanes)
            added = jnp.where(rows + k * SUBS < depth, horizontal_rate * flat[k], 0.0)
            out[at] = part[at] + tracer_step * added
        return carry

    lax.fori_loop(0, blocks, cell_block, 0)


def shards(
    tracer, bottom_levels, neighbours, edge_weight, ssh, velocity, send_blocks, thickness, profile
):
    count = lax.axis_size("dom")
    levels, cells = tracer.shape
    send = send_blocks.shape[-1]
    edges = neighbours.shape[0]
    blocks = cells // LANES
    assert blocks == SUBS and 4 * send == SUBS and levels % SUBS == 0 and count % (2 * TEAM) == 0
    assert SUBSTEPS == 6
    tile = (blocks, LANES)
    place = lax.axis_index("dom").astype(jnp.int32)[None]
    slots = jnp.swapaxes(send_blocks, 1, 2)
    bottom = bottom_levels.reshape(tile)

    def shape(rows, kind=jnp.float32):
        return jax.ShapeDtypeStruct(rows, kind)

    def call(body, outs, ins, scratch, flops, limit=4):
        return pl.pallas_call(
            functools.partial(body, send=send),
            out_shape=outs,
            in_specs=ins,
            scratch_shapes=scratch,
            compiler_params=pltpu.CompilerParams(vmem_limit_bytes=limit << 20),
            cost_estimate=pl.CostEstimate(flops=flops, bytes_accessed=1000, transcendentals=0),
        )

    own = (2 * edges + 4) * SUBS
    halo = send * levels
    near, side, far = call(
        functools.partial(prepare, count=count),
        [
            shape((own + halo, LANES)),
            shape((own + halo, LANES)),
            shape((own, LANES)),
        ],
        [SMEM, SMEM, SMEM] + [VMEM] * 6,
        [],
        4000000,
        60,
    )(
        place, slots, thickness, tracer, bottom, neighbours, edge_weight, ssh.reshape(tile),
        velocity.reshape(tile),
    )
    part, columns, mine, odd, odd_side, local = call(
        functools.partial(tracer_own, count=count),
        [
            shape(tracer.shape),
            shape((levels, LANES)),
            shape((own, LANES)),
            shape((halo, LANES)),
            shape((halo, LANES)),
            shape(neighbours.shape, jnp.int32),
        ],
        [SMEM] * 4 + [VMEM] * 6,
        [pltpu.VMEM(tracer.shape, jnp.float32)],
        10000000,
    )(
        place, slots, thickness, profile, tracer, bottom, neighbours, edge_weight,
        ssh.reshape(tile), velocity.reshape(tile),
    )

    def send_on(value, way):
        return lax.ppermute(value, "dom", way)

    side = send_on(side, even_swap(count, 2))
    far = send_on(far, even_swap(count, 3))
    near = send_on(near, even_swap(count, 1))
    odd = send_on(odd, odd_swap(count, 1))
    odd_side = send_on(odd_side, odd_swap(count, 2))

    def swap(pair):
        return (send_on(pair[0], even_swap(count, TEAM)), send_on(pair[1], odd_swap(count, TEAM)))

    state = [shape((TEAM,) + tile)] * 2
    entire = (6 + 2 * edges + 1) * SUBS
    *tables, height, speed, way_even, way_odd = call(
        gather_team,
        [
            shape((TEAM, edges) + tile, jnp.int32),
            shape((TEAM, edges) + tile),
            shape((TEAM,) + tile),
            shape((TEAM,) + tile, jnp.int32),
        ]
        + state
        + [shape((entire, LANES))] * 2,
        [SMEM] + [VMEM] * 4,
        [],
        500000,
    )(place, mine, near, side, far)
    constant = swap((way_even, way_odd))
    base = part
    for ways, pair in (((0, 2), (near, side)), ((1, 3), (odd, odd_side))):
        base = call(
            functools.partial(tracer_halo, ways=ways), shape(tracer.shape), [VMEM] * 7, [], 5000000
        )(tracer, bottom, local, edge_weight, base, *pair)
    scratch = [pltpu.VMEM((TEAM, 2 * SUBS, LANES), jnp.float32)] * 2
    light = [shape((6 * SUBS, LANES))] * 2
    height, speed, total, *ways = call(
        first_pair, state + state[:1] + light, [SMEM] + [VMEM] * 8, scratch, 2000000
    )(place, *tables, height, speed, *constant)
    arrived = swap(ways)
    height, speed, total, *ways = call(
        middle_pair, state + state[:1] + light, [SMEM] + [VMEM] * 11, scratch, 2000000
    )(place, *tables, height, speed, total, *arrived, *constant)
    arrived = swap(ways)
    team_scratch = [pltpu.VMEM((TEAM,) + tile, jnp.float32)] * 3
    height, speed, result = pl.pallas_call(
        functools.partial(last_pair, send=send),
        out_shape=[shape(tile), shape(tile), shape(tracer.shape)],
        in_specs=[SMEM] + [VMEM] * 14,
        out_specs=[HBM, HBM, HBM],
        scratch_shapes=[pltpu.VMEM(tracer.shape, jnp.float32)]
        + team_scratch
        + scratch
        + [pltpu.SemaphoreType.DMA((levels // SUBS + 2,))],
        compiler_params=pltpu.CompilerParams(vmem_limit_bytes=4 << 20),
        cost_estimate=pl.CostEstimate(flops=2500000, bytes_accessed=1000, transcendentals=0),
        name="last_pair",
    )(place, *tables, height, speed, total, *arrived, *constant, bottom, base, columns)
    return (result, height.reshape(-1), speed.reshape(-1))


def solution(mesh):
    placed = (
        P(None, "dom"),
        P("dom"),
        P(None, "dom"),
        P(None, "dom"),
        P("dom"),
        P("dom"),
        P("dom", None, None),
        P(),
        P(),
    )

    return jax.shard_map(
        shards,
        mesh=mesh,
        in_specs=placed,
        out_specs=(P(None, "dom"), P("dom"), P("dom")),
        check_vma=False,
    )
```

```python
import functools

import jax
import jax.numpy as jnp
from jax import lax
from jax.experimental import pallas as pl
from jax.experimental.pallas import tpu as pltpu
from jax.sharding import PartitionSpec as P


LANES = 128
SUBS = 8
SUBSTEPS = 6
TEAM = 4
OFFSETS = (1, -1, 2, -2)
horizontal_rate = 0.5
vertical_rate = 0.5
tracer_step = 0.2
barotropic_step = 0.5
friction = 0.05
ABSENT = 3e38
PRESENT = 1e38


SMEM = pl.BlockSpec(memory_space=pltpu.SMEM)
VMEM = pl.BlockSpec(memory_space=pltpu.VMEM)
HBM = pl.BlockSpec(memory_space=pltpu.HBM)


def even_swap(count, by):
    return [(i, i ^ by) for i in range(count)]


def odd_swap(count, by):
    pairs = [(i, i + by) for i in range(by, count - by) if (i // by) % 2 == 1]
    pairs += [(b, a) for a, b in pairs]
    busy = {a for a, _ in pairs}
    rest = [i for i in range(count) if i not in busy]
    pairs += list(zip(rest[0::2], rest[1::2])) + list(zip(rest[1::2], rest[0::2]))
    return pairs


def column(scalars, tile):
    rows = lax.broadcasted_iota(jnp.int32, (SUBS, LANES), 0)
    value = jnp.zeros((SUBS, LANES), jnp.float32)
    for k in range(SUBS):
        value = jnp.where(rows == k, scalars[tile * SUBS + k], value)
    return value


def localize(index, place, count, cells, send):
    span = send * LANES
    result = index
    for g, offset in enumerate(OFFSETS):
        source = place - offset
        inside = jnp.logical_and(source >= 0, source < count)
        swapped = (place // abs(offset)) % 2 == 0
        step = jnp.where(swapped, span if g % 2 == 0 else -span, 0)
        low = cells + g * span
        mine = jnp.logical_and(index >= low, index < low + span)
        moved = jnp.where(inside, index + step, cells + 4 * span)
        result = jnp.where(mine, moved, result)
    return result


def group_of(rows, send):
    return rows // send


def blend(rows, send, parts):
    value = jnp.zeros((SUBS, LANES), jnp.float32)
    for g, part in parts.items():
        value = jnp.where(group_of(rows, send) == g, part, value)
    return value


def outgoing(field, slots):
    taken = jnp.take_along_axis(field, jnp.maximum(slots, 0), axis=0)
    return jnp.where(slots >= 0, taken, 0.0)


def tracer_blocks(place, slots, tracer, bottom, outs, send):
    levels = tracer.shape[0]
    tiles = levels // SUBS
    rows = lax.broadcasted_iota(jnp.int32, (SUBS, LANES), 0)
    for way, out in outs:
        offset = 1 if way < 2 else 2
        first = (place // offset) % 2 == 0
        base = 0 if way < 2 else 2
        start = out.shape[0] - send * levels
        for slot in range(send):
            block = jnp.where(
                first, slots[0, slot, base + way % 2], slots[0, slot, base + 1 - way % 2]
            )
            safe = jnp.maximum(block, 0)
            depth = jnp.where(block >= 0, bottom[pl.ds(safe, 1), :], 0)
            at = pl.multiple_of(safe * LANES, LANES)
            for k in range(tiles):
                value = tracer[k * SUBS : (k + 1) * SUBS, pl.ds(at, LANES)]
                row = start + slot * levels + k * SUBS
                out[row : row + SUBS, :] = jnp.where(rows + k * SUBS < depth, value, ABSENT)


def prepare(
    place_ref, slots, thick, tracer, bottom, index, weight, ssh, velocity, near, side, far, mine, by_one,
    by_two, sems, *, count, send,
):
    place = place_ref[0]
    own = mine.shape[0]
    tracer_blocks(place, slots, tracer, bottom, ((0, by_one), (2, by_two)), send)
    copies = [
        pltpu.make_async_copy(by_two, side.at[own:, :], sems.at[0]),
        pltpu.make_async_copy(by_one, near.at[own:, :], sems.at[1]),
    ]
    for copy in copies:
        copy.start()
    own_tables(place, slots, thick, tracer, bottom, index, weight, ssh, velocity, mine, count, send)
    late = [
        pltpu.make_async_copy(mine, side.at[:own, :], sems.at[2]),
        pltpu.make_async_copy(mine, far, sems.at[3]),
        pltpu.make_async_copy(mine, near.at[:own, :], sems.at[4]),
    ]
    for copy in late:
        copy.start()
    for copy in copies + late:
        copy.wait()


def own_tables(
    place, slots, thick, tracer, bottom, index, weight, ssh, velocity, mine, count, send
):
    levels, cells = tracer.shape
    tiles = levels // SUBS
    blocks = cells // LANES
    edges = index.shape[0]
    rows = lax.broadcasted_iota(jnp.int32, (SUBS, LANES), 0)
    thicks = [column(thick, k) for k in range(tiles)]
    sent = jnp.zeros((SUBS, LANES), jnp.float32)
    for g in range(4):
        for slot in range(send):
            sent = jnp.where(rows == g * send + slot, slots[0, slot, g].astype(jnp.float32), sent)
    team = (2 * edges + 3) * SUBS
    mine[team : team + SUBS, :] = sent
    for b in range(blocks):
        top = jnp.zeros((SUBS, LANES), jnp.float32)
        low = jnp.zeros((SUBS, LANES), jnp.float32)
        depth = bottom[b : b + 1, :]
        for k in range(tiles):
            layer = jnp.where(rows + k * SUBS < depth, thicks[k], 0.0)
            top = top + layer * tracer[k * SUBS : (k + 1) * SUBS, b * LANES : (b + 1) * LANES]
            low = low + layer
        row = 2 * edges * SUBS + b
        mine[row : row + 1, :] = jnp.sum(top, axis=0, keepdims=True) / jnp.sum(
            low, axis=0, keepdims=True
        )
    for b in range(blocks):
        lanes = slice(b * LANES, (b + 1) * LANES)
        for j in range(edges):
            row = j * SUBS + b
            mine[row : row + 1, :] = index[j : j + 1, lanes].astype(jnp.float32)
            row = (edges + j) * SUBS + b
            mine[row : row + 1, :] = weight[j : j + 1, lanes]
    for j in range(edges):
        at = slice(j * SUBS, (j + 1) * SUBS)
        mine[at, :] = bounded(mine[at, :], place, count, cells, send)
    row = (2 * edges + 1) * SUBS
    mine[row : row + SUBS, :] = velocity[...]
    mine[row + SUBS : row + 2 * SUBS, :] = ssh[...]


def bounded(index, place, count, cells, send):
    span = send * LANES
    result = index
    for g, offset in enumerate(OFFSETS):
        source = place - offset
        inside = jnp.logical_and(source >= 0, source < count)
        low = jnp.where(inside, cells + 4 * span, cells + g * span)
        low = low.astype(index.dtype)
        mine = jnp.logical_and(index >= low, index < cells + (g + 1) * span)
        result = jnp.where(mine, jnp.asarray(cells + 4 * span, index.dtype), result)
    return result


def gathered(rows_of, index, weight, own, pairs):
    laplace = jnp.zeros_like(own)
    for j in range(len(index)):
        lane = jnp.bitwise_and(index[j], LANES - 1)
        block = jnp.right_shift(index[j], 7)
        got = jnp.zeros_like(own)
        for r in range(pairs):
            got = jnp.where(block == r, jnp.take_along_axis(rows_of(r), lane, axis=1), got)
        laplace = laplace + weight[j] * (got - own)
    return laplace


def stepped(laplace, forcing, own, speed):
    faster = (1.0 - friction) * speed + barotropic_step * (laplace + forcing)
    return own + barotropic_step * faster, faster


def pack_edges(heights, speeds, slots, rows, send, even, way_even, way_odd):
    out = [outgoing(h, s) for h, s in zip(heights, slots)]
    fast = [outgoing(v, slots[q]) for q, v in enumerate(speeds)]
    right = [
        heights[3],
        heights[2],
        blend(rows, send, {0: out[2], 2: out[1]}),
        blend(rows, send, {0: out[1], 1: out[3], 2: out[0]}),
        edge_rows(out[3], out[2], rows, send, True),
        edge_rows(fast[3], fast[2], rows, send, True),
    ]
    left = [
        heights[0],
        heights[1],
        blend(rows, send, {1: out[1], 3: out[2]}),
        blend(rows, send, {0: out[0], 1: out[2], 3: out[3]}),
        edge_rows(out[0], out[1], rows, send, False),
        edge_rows(fast[0], fast[1], rows, send, False),
    ]
    for k in range(len(right)):
        at = slice(k * SUBS, (k + 1) * SUBS)
        way_even[at, :] = jnp.where(even, right[k], left[k])
        way_odd[at, :] = jnp.where(even, left[k], right[k])


def edge_rows(inner, outer, rows, send, rightward):
    if rightward:
        return jnp.where(group_of(rows, send) == 3, pltpu.roll(outer, send, 0), inner)
    return jnp.where(group_of(rows, send) == 2, pltpu.roll(outer, SUBS - send, 0), inner)


def gather_team(
    place_ref, mine, near, side, far, index, weight, force, slots, height, speed, way_even, way_odd,
    *, send,
):
    edges = index.shape[1]
    place = place_ref[0]
    position = place % TEAM
    even = (place // TEAM) % 2 == 0
    rows = lax.broadcasted_iota(jnp.int32, (SUBS, LANES), 0)
    for flip, ref in enumerate((mine, near, side, far)):
        q = jnp.bitwise_xor(position, flip)
        for j in range(edges):
            index[q, j] = ref[j * SUBS : (j + 1) * SUBS, :].astype(jnp.int32)
            weight[q, j] = ref[(edges + j) * SUBS : (edges + j + 1) * SUBS, :]
        row = 2 * edges * SUBS
        force[q] = ref[row : row + SUBS, :]
        speed[q] = ref[row + SUBS : row + 2 * SUBS, :]
        height[q] = ref[row + 2 * SUBS : row + 3 * SUBS, :]
        slots[q] = ref[row + 3 * SUBS : row + 4 * SUBS, :].astype(jnp.int32)
    held = [slots[q] for q in range(TEAM)]
    pack_edges(
        [height[q] for q in range(TEAM)], [speed[q] for q in range(TEAM)], held, rows, send, even,
        way_even, way_odd,
    )

    def both(k, field):
        at = slice((6 + k) * SUBS, (7 + k) * SUBS)
        picked = [outgoing(field(q), held[q]) for q in range(TEAM)]
        right = edge_rows(picked[3], picked[2], rows, send, True)
        left = edge_rows(picked[0], picked[1], rows, send, False)
        way_even[at, :] = jnp.where(even, right, left)
        way_odd[at, :] = jnp.where(even, left, right)

    for j in range(edges):
        both(j, lambda q: index[q, j].astype(jnp.float32))
        both(edges + j, lambda q: weight[q, j])
    both(2 * edges, lambda q: force[q])


def double_step(
    place, index, weight, force, slots, height_in, speed_in, total_in, even_in, odd_in, first_even,
    first_odd, height, speed, total, ext, virtual, only, *, send,
):
    edges = index.shape[1]
    even = (place // TEAM) % 2 == 0
    rows = lax.broadcasted_iota(jnp.int32, (SUBS, LANES), 0)
    held = [slots[q] for q in range(TEAM)]

    def side_of(k, constant, right):
        ref_even, ref_odd = (first_even, first_odd) if constant else (even_in, odd_in)
        at = slice(k * SUBS, (k + 1) * SUBS)
        a, b = ref_even[at, :], ref_odd[at, :]
        return jnp.where(even == right, a, b)

    def fill(heights, left, right):
        out = [outgoing(h, s) for h, s in zip(heights, held)]
        halos = (
            {0: left, 1: out[1], 2: pltpu.roll(left, SUBS - send, 0), 3: out[2]},
            {0: out[0], 1: out[2], 2: left, 3: out[3]},
            {0: out[1], 1: out[3], 2: out[0], 3: right},
            {0: out[2], 1: right, 2: out[1], 3: pltpu.roll(right, send, 0)},
        )
        for q in range(TEAM):
            ext[q, 0:SUBS, :] = heights[q]
            ext[q, SUBS : 2 * SUBS, :] = blend(rows, send, halos[q])
        return out

    def advance_team(heights, speeds):
        moved = []
        for q in range(TEAM):
            laplace = gathered(
                lambda r: jnp.broadcast_to(ext[q, r : r + 1, :], (SUBS, LANES)),
                [index[q, j] for j in range(edges)],
                [weight[q, j] for j in range(edges)],
                heights[q],
                2 * SUBS,
            )
            moved.append(stepped(laplace, force[q], heights[q], speeds[q]))
        return [m[0] for m in moved], [m[1] for m in moved]

    heights = [height_in[q] for q in range(TEAM)]
    speeds = [speed_in[q] for q in range(TEAM)]
    edge = [side_of(4, False, right) for right in (False, True)]
    out = fill(heights, edge[0], edge[1])
    virtual[0, 0:SUBS, :] = side_of(0, False, False)
    virtual[0, SUBS : 2 * SUBS, :] = side_of(2, False, False) + blend(
        rows, send, {1: out[0], 3: out[1]}
    )
    virtual[1, 0:SUBS, :] = side_of(1, False, False)
    virtual[1, SUBS : 2 * SUBS, :] = side_of(3, False, False) + blend(rows, send, {3: out[0]})
    virtual[2, 0:SUBS, :] = side_of(0, False, True)
    virtual[2, SUBS : 2 * SUBS, :] = side_of(2, False, True) + blend(
        rows, send, {0: out[3], 2: out[2]}
    )
    virtual[3, 0:SUBS, :] = side_of(1, False, True)
    virtual[3, SUBS : 2 * SUBS, :] = side_of(3, False, True) + blend(rows, send, {2: out[3]})
    later, faster = advance_team(heights, speeds)
    if only is None:
        wanted = ((0, False), (1, True))
    else:
        right = only >= TEAM // 2
        wanted = ((right.astype(jnp.int32), right),)
    moved_edges = []
    for number, right in wanted:
        before = jnp.where(right, edge[1], edge[0])
        moved_group = jnp.where(right, 2, 3)
        laplace = gathered(
            lambda r: jnp.where(
                group_of(rows, send) == moved_group,
                virtual[2 * number + 1, r : r + 1, :],
                virtual[2 * number, r : r + 1, :],
            ),
            [side_of(6 + j, True, right).astype(jnp.int32) for j in range(edges)],
            [side_of(6 + edges + j, True, right) for j in range(edges)],
            before,
            2 * SUBS,
        )
        force_here = side_of(6 + 2 * edges, True, right)
        moved_edges.append(stepped(laplace, force_here, before, side_of(5, False, right))[0])
    edge = [moved_edges[0], moved_edges[-1]]
    fill(later, edge[0], edge[1])
    if only is not None:
        for q in range(TEAM):
            height[q] = later[q]
            speed[q] = faster[q]
        q = only
        laplace = gathered(
            lambda r: jnp.broadcast_to(ext[q, r : r + 1, :], (SUBS, LANES)),
            [index[q, j] for j in range(edges)],
            [weight[q, j] for j in range(edges)],
            height[q],
            2 * SUBS,
        )
        before = total_in[q] + speed[q]
        height[q], speed[q] = stepped(laplace, force[q], height[q], speed[q])
        total[q] = before + speed[q]
        return None
    last, fastest = advance_team(later, faster)
    for q in range(TEAM):
        height[q] = last[q]
        speed[q] = fastest[q]
        before = 0.0 if total_in is None else total_in[q]
        total[q] = before + faster[q] + fastest[q]
    return last, fastest, held, rows, even


def first_pair(
    place, index, weight, force, slots, height_in, speed_in, even_in, odd_in, height, speed, total,
    way_even, way_odd, ext, virtual, *, send,
):
    last, fastest, held, rows, even = double_step(
        place[0], index, weight, force, slots, height_in, speed_in, None, even_in, odd_in, even_in,
        odd_in, height, speed, total, ext, virtual, None, send=send,
    )
    pack_edges(last, fastest, held, rows, send, even, way_even, way_odd)


def middle_pair(
    place, index, weight, force, slots, height_in, speed_in, total_in, even_in, odd_in, first_even,
    first_odd, height, speed, total, way_even, way_odd, ext, virtual, *, send,
):
    last, fastest, held, rows, even = double_step(
        place[0], index, weight, force, slots, height_in, speed_in, total_in, even_in, odd_in,
        first_even, first_odd, height, speed, total, ext, virtual, None, send=send,
    )
    pack_edges(last, fastest, held, rows, send, even, way_even, way_odd)


def last_pair(
    place_ref, index, weight, force, slots, height_in, speed_in, total_in, even_in, odd_in,
    first_even, first_odd, bottom, base, shape, height_hbm, speed_hbm, out_hbm, out, height, speed,
    total, ext, virtual, sems, *, send,
):
    position = place_ref[0] % TEAM
    double_step(
        place_ref[0], index, weight, force, slots, height_in, speed_in, total_in, even_in, odd_in,
        first_even, first_odd, height, speed, total, ext, virtual, position, send=send,
    )
    ext[0, 0:SUBS, :] = total[position] / SUBSTEPS
    rows = lax.broadcasted_iota(jnp.int32, (SUBS, LANES), 0)
    tiles = out.shape[0] // SUBS
    copies = [
        pltpu.make_async_copy(height.at[position], height_hbm, sems.at[tiles]),
        pltpu.make_async_copy(speed.at[position], speed_hbm, sems.at[tiles + 1]),
    ]
    for copy in copies:
        copy.start()
    for k in range(out.shape[0] // SUBS):
        levels = slice(k * SUBS, (k + 1) * SUBS)
        for i in range(out.shape[1] // LANES):
            at = (levels, slice(i * LANES, (i + 1) * LANES))
            added = jnp.where(rows + k * SUBS < bottom[i : i + 1, :], shape[levels, :], 0.0)
            out[at] = base[at] + added * ext[0, i : i + 1, :]
        copies.append(
            pltpu.make_async_copy(out.at[levels, :], out_hbm.at[levels, :], sems.at[k])
        )
        copies[-1].start()
    for copy in copies:
        copy.wait()


def collected(sources, index, weight, mine, tiles):
    flat = [jnp.zeros((SUBS, LANES), jnp.float32) for _ in range(tiles)]
    for near, factor in zip(index, weight):
        near = jnp.broadcast_to(near, (SUBS, LANES))
        lane = jnp.bitwise_and(near, LANES - 1)
        block = jnp.right_shift(near, 7)
        got = [jnp.full((SUBS, LANES), ABSENT, jnp.float32) for _ in range(tiles)]
        for r, source in sources:
            here = block == r
            for k in range(tiles):
                found = jnp.take_along_axis(source(k), lane, axis=1)
                got[k] = jnp.where(here, found, got[k])
        for k in range(tiles):
            flat[k] = flat[k] + factor * jnp.where(got[k] < PRESENT, got[k] - mine[k], 0.0)
    return flat


def tracer_own(
    place_ref, slots, thick, profile, tracer, bottom, index, weight, ssh, velocity, out, shape, mine_out,
    odd, odd_side, local, held, *, count, send,
):
    own_tables(
        place_ref[0], slots, thick, tracer, bottom, index, weight, ssh, velocity, mine_out, count, send
    )
    tracer_blocks(place_ref[0], slots, tracer, bottom, ((1, odd), (3, odd_side)), send)
    for i in range(index.shape[1] // LANES):
        at = slice(i * LANES, (i + 1) * LANES)
        local[:, at] = localize(index[:, at], place_ref[0], count, index.shape[1], send)
    levels, cells = tracer.shape
    tiles = levels // SUBS
    blocks = cells // LANES
    edges = index.shape[0]
    rows = lax.broadcasted_iota(jnp.int32, (SUBS, LANES), 0)
    for i in range(blocks):
        depth = bottom[i : i + 1, :]
        for k in range(tiles):
            at = (slice(k * SUBS, (k + 1) * SUBS), slice(i * LANES, (i + 1) * LANES))
            held[at] = jnp.where(rows + k * SUBS < depth, tracer[at], ABSENT)
    for k in range(tiles):
        shape[k * SUBS : (k + 1) * SUBS, :] = column(profile, k)

    def source(r):
        return lambda k: held[k * SUBS : (k + 1) * SUBS, r * LANES : (r + 1) * LANES]

    def cell_block(i, carry):
        lanes = pl.ds(pl.multiple_of(i * LANES, LANES), LANES)
        depth = bottom[pl.ds(i, 1), :]
        mine = [tracer[k * SUBS : (k + 1) * SUBS, lanes] for k in range(tiles)]
        flat = collected(
            [(r, source(r)) for r in range(blocks)],
            [index[j : j + 1, lanes] for j in range(edges)],
            [weight[j : j + 1, lanes] for j in range(edges)],
            mine,
            tiles,
        )
        for k in range(tiles):
            first = rows + k * SUBS
            value = mine[k]
            up = pltpu.roll(value, SUBS - 1, 0)
            if k + 1 < tiles:
                up = jnp.where(rows == SUBS - 1, pltpu.roll(mine[k + 1], SUBS - 1, 0), up)
            down = pltpu.roll(value, 1, 0)
            if k > 0:
                down = jnp.where(rows == 0, pltpu.roll(mine[k - 1], 1, 0), down)
            below = jnp.where(first + 1 < jnp.minimum(depth, levels), up - value, 0.0)
            above = jnp.where(first > 0, down - value, 0.0)
            moved = horizontal_rate * flat[k] + vertical_rate * (below + above)
            out[k * SUBS : (k + 1) * SUBS, lanes] = value + tracer_step * jnp.where(
                first < depth, moved, 0.0
            )
        return carry

    lax.fori_loop(0, blocks, cell_block, 0)


def tracer_halo(tracer, bottom, local, weight, part, a, b, out, *, send, ways):
    levels, cells = tracer.shape
    tiles = levels // SUBS
    blocks = cells // LANES
    edges = local.shape[0]
    rows = lax.broadcasted_iota(jnp.int32, (SUBS, LANES), 0)

    def source(ref, slot):
        start = ref.shape[0] - send * levels + slot * levels
        return lambda k: ref[start + k * SUBS : start + (k + 1) * SUBS, :]

    sources = [
        (blocks + way * send + slot, source(ref, slot))
        for way, ref in zip(ways, (a, b))
        for slot in range(send)
    ]

    def cell_block(i, carry):
        lanes = pl.ds(pl.multiple_of(i * LANES, LANES), LANES)
        depth = bottom[pl.ds(i, 1), :]
        mine = [tracer[k * SUBS : (k + 1) * SUBS, lanes] for k in range(tiles)]
        near = [local[j : j + 1, lanes] for j in range(edges)]
        factors = [weight[j : j + 1, lanes] for j in range(edges)]
        flat = collected(sources, near, factors, mine, tiles)
        for k in range(tiles):
            at = (slice(k * SUBS, (k + 1) * SUBS), lanes)
            added = jnp.where(rows + k * SUBS < depth, horizontal_rate * flat[k], 0.0)
            out[at] = part[at] + tracer_step * added
        return carry

    lax.fori_loop(0, blocks, cell_block, 0)


def shards(
    tracer, bottom_levels, neighbours, edge_weight, ssh, velocity, send_blocks, thickness, profile
):
    count = lax.axis_size("dom")
    levels, cells = tracer.shape
    send = send_blocks.shape[-1]
    edges = neighbours.shape[0]
    blocks = cells // LANES
    assert blocks == SUBS and 4 * send == SUBS and levels % SUBS == 0 and count % (2 * TEAM) == 0
    assert SUBSTEPS == 6
    tile = (blocks, LANES)
    place = lax.axis_index("dom").astype(jnp.int32)[None]
    slots = jnp.swapaxes(send_blocks, 1, 2)
    bottom = bottom_levels.reshape(tile)

    def shape(rows, kind=jnp.float32):
        return jax.ShapeDtypeStruct(rows, kind)

    def call(body, outs, ins, scratch, flops, limit=4, placed=None):
        if placed is None:
            placed = jax.tree.map(lambda _: VMEM, outs)
        return pl.pallas_call(
            functools.partial(body, send=send),
            out_shape=outs,
            in_specs=ins,
            out_specs=placed,
            scratch_shapes=scratch,
            compiler_params=pltpu.CompilerParams(vmem_limit_bytes=limit << 20),
            cost_estimate=pl.CostEstimate(flops=flops, bytes_accessed=1000, transcendentals=0),
        )

    own = (2 * edges + 4) * SUBS
    halo = send * levels
    near, side, far = call(
        functools.partial(prepare, count=count),
        [
            shape((own + halo, LANES)),
            shape((own + halo, LANES)),
            shape((own, LANES)),
        ],
        [SMEM, SMEM, SMEM] + [VMEM] * 6,
        [
            pltpu.VMEM((own, LANES), jnp.float32),
            pltpu.VMEM((halo, LANES), jnp.float32),
            pltpu.VMEM((halo, LANES), jnp.float32),
            pltpu.SemaphoreType.DMA((5,)),
        ],
        4000000,
        60,
        [HBM] * 3,
    )(
        place, slots, thickness, tracer, bottom, neighbours, edge_weight, ssh.reshape(tile),
        velocity.reshape(tile),
    )
    part, columns, mine, odd, odd_side, local = call(
        functools.partial(tracer_own, count=count),
        [
            shape(tracer.shape),
            shape((levels, LANES)),
            shape((own, LANES)),
            shape((halo, LANES)),
            shape((halo, LANES)),
            shape(neighbours.shape, jnp.int32),
        ],
        [SMEM] * 4 + [VMEM] * 6,
        [pltpu.VMEM(tracer.shape, jnp.float32)],
        10000000,
    )(
        place, slots, thickness, profile, tracer, bottom, neighbours, edge_weight,
        ssh.reshape(tile), velocity.reshape(tile),
    )

    def send_on(value, way):
        return lax.ppermute(value, "dom", way)

    side = send_on(side, even_swap(count, 2))
    far = send_on(far, even_swap(count, 3))
    near = send_on(near, even_swap(count, 1))
    odd = send_on(odd, odd_swap(count, 1))
    odd_side = send_on(odd_side, odd_swap(count, 2))

    def swap(pair):
        return (send_on(pair[0], even_swap(count, TEAM)), send_on(pair[1], odd_swap(count, TEAM)))

    state = [shape((TEAM,) + tile)] * 2
    entire = (6 + 2 * edges + 1) * SUBS
    *tables, height, speed, way_even, way_odd = call(
        gather_team,
        [
            shape((TEAM, edges) + tile, jnp.int32),
            shape((TEAM, edges) + tile),
            shape((TEAM,) + tile),
            shape((TEAM,) + tile, jnp.int32),
        ]
        + state
        + [shape((entire, LANES))] * 2,
        [SMEM] + [VMEM] * 4,
        [],
        500000,
    )(place, mine, near, side, far)
    constant = swap((way_even, way_odd))
    base = part
    for ways, pair in (((0, 2), (near, side)), ((1, 3), (odd, odd_side))):
        base = call(
            functools.partial(tracer_halo, ways=ways), shape(tracer.shape), [VMEM] * 7, [], 5000000
        )(tracer, bottom, local, edge_weight, base, *pair)
    scratch = [pltpu.VMEM((TEAM, 2 * SUBS, LANES), jnp.float32)] * 2
    light = [shape((6 * SUBS, LANES))] * 2
    height, speed, total, *ways = call(
        first_pair, state + state[:1] + light, [SMEM] + [VMEM] * 8, scratch, 2000000
    )(place, *tables, height, speed, *constant)
    arrived = swap(ways)
    height, speed, total, *ways = call(
        middle_pair, state + state[:1] + light, [SMEM] + [VMEM] * 11, scratch, 2000000
    )(place, *tables, height, speed, total, *arrived, *constant)
    arrived = swap(ways)
    team_scratch = [pltpu.VMEM((TEAM,) + tile, jnp.float32)] * 3
    height, speed, result = pl.pallas_call(
        functools.partial(last_pair, send=send),
        out_shape=[shape(tile), shape(tile), shape(tracer.shape)],
        in_specs=[SMEM] + [VMEM] * 14,
        out_specs=[HBM, HBM, HBM],
        scratch_shapes=[pltpu.VMEM(tracer.shape, jnp.float32)]
        + team_scratch
        + scratch
        + [pltpu.SemaphoreType.DMA((levels // SUBS + 2,))],
        compiler_params=pltpu.CompilerParams(vmem_limit_bytes=4 << 20),
        cost_estimate=pl.CostEstimate(flops=2500000, bytes_accessed=1000, transcendentals=0),
        name="last_pair",
    )(place, *tables, height, speed, total, *arrived, *constant, bottom, base, columns)
    return (result, height.reshape(-1), speed.reshape(-1))


def solution(mesh):
    placed = (
        P(None, "dom"),
        P("dom"),
        P(None, "dom"),
        P(None, "dom"),
        P("dom"),
        P("dom"),
        P("dom", None, None),
        P(),
        P(),
    )

    return jax.shard_map(
        shards,
        mesh=mesh,
        in_specs=placed,
        out_specs=(P(None, "dom"), P("dom"), P("dom")),
        check_vma=False,
    )
```
